16 devices in a mesh: sp: 2 (over z), fsdp: 8 (over y, x, core).
Axes of the slice: x: 2, y: 2, z: 2, core: 2. Of those that a mesh axis runs over, the one named last changes fastest.
Arguments:
- x: bfloat16 [128, 512, 2048], P('fsdp', 'sp')
- grad_y: bfloat16 [128, 512, 2048], P('fsdp', 'sp')
- w_q: bfloat16 [2048, 2048], P('fsdp')
- w_k: bfloat16 [2048, 2048], P('fsdp')
- w_v: bfloat16 [2048, 2048], P('fsdp')
- w_o: bfloat16 [2048, 2048], P('fsdp')
- q_norm_w: float32 [2048], P('fsdp')
- k_norm_w: float32 [2048], P('fsdp')
- post_norm_w: float32 [2048], P('fsdp')
Outputs:
- output 1: bfloat16 [128, 512, 2048], P('fsdp', 'sp')
- output 2: bfloat16 [128, 512, 2048], P('fsdp', 'sp')
- output 3: float32 [2048, 2048], P('fsdp')
- output 4: float32 [2048, 2048], P('fsdp')
- output 5: float32 [2048, 2048], P('fsdp')
- output 6: float32 [2048, 2048], P('fsdp')
- output 7: float32 [2048], P('fsdp')
- output 8: float32 [2048], P('fsdp')
- output 9: float32 [2048], P('fsdp')
All inputs are finite; a program needn't handle non-finite values.
Results may differ from the reference program's by a relative error of at most 0.0131786.
Values are sent between devices in bfloat16 or wider.
A program may use at most 1 GiB of HBM per device.

```python
import jax
import jax.numpy as jnp
from jax import lax

BATCH_SIZE = 128
SEQ_LEN = 512
D_MODEL = 2048
N_HEADS = 16
HEAD_DIM = 128
RMS_EPSILON = 1e-6
ROPE_THETA = 500000.0


def setup_inputs(seed: int = 0) -> dict:
    key_list = jax.random.split(jax.random.key(seed), 11)
    tok_shape = (BATCH_SIZE, SEQ_LEN, D_MODEL)
    fan_scale = D_MODEL ** -0.5
    q_scale = jnp.repeat(jnp.exp(jax.random.uniform(key_list[0], (N_HEADS,), jnp.float32, -0.7, 0.7)), HEAD_DIM)
    k_scale = jnp.repeat(jnp.exp(jax.random.uniform(key_list[1], (N_HEADS,), jnp.float32, -0.7, 0.7)), HEAD_DIM)
    x = jax.random.normal(key_list[2], tok_shape, jnp.float32)
    grad_y = jax.random.normal(key_list[3], tok_shape, jnp.float32)
    w_q = jax.random.normal(key_list[4], (D_MODEL, D_MODEL), jnp.float32) * (fan_scale * q_scale)[None, :]
    w_k = jax.random.normal(key_list[5], (D_MODEL, D_MODEL), jnp.float32) * (fan_scale * k_scale)[None, :]
    w_v = jax.random.normal(key_list[6], (D_MODEL, D_MODEL), jnp.float32) * fan_scale
    w_o = jax.random.normal(key_list[7], (D_MODEL, D_MODEL), jnp.float32) * fan_scale
    q_norm_w = jax.random.uniform(key_list[8], (D_MODEL,), jnp.float32, 0.6, 1.4)
    k_norm_w = jax.random.uniform(key_list[9], (D_MODEL,), jnp.float32, 0.6, 1.4)
    post_norm_w = jax.random.uniform(key_list[10], (D_MODEL,), jnp.float32, 0.6, 1.4)
    return {'x': x.astype(jnp.bfloat16), 'grad_y': grad_y.astype(jnp.bfloat16), 'w_q': w_q.astype(jnp.bfloat16), 'w_k': w_k.astype(jnp.bfloat16), 'w_v': w_v.astype(jnp.bfloat16), 'w_o': w_o.astype(jnp.bfloat16), 'q_norm_w': q_norm_w, 'k_norm_w': k_norm_w, 'post_norm_w': post_norm_w}


def snap_bf16(values):
    rounded = values.astype(jnp.bfloat16).astype(values.dtype)
    return values + lax.stop_gradient(rounded - values)


def rms_norm(values, gain_vec):
    inv_rms = lax.rsqrt(jnp.mean(values * values, axis=-1, keepdims=True) + RMS_EPSILON)
    return values * inv_rms * gain_vec


def rope_tables():
    half_dim = HEAD_DIM // 2
    inv_freq = ROPE_THETA ** (-jnp.arange(half_dim, dtype=jnp.float32) * (2.0 / HEAD_DIM))
    angles = jnp.arange(SEQ_LEN, dtype=jnp.float32)[:, None] * inv_freq[None, :]
    return jnp.cos(angles)[:, None, :], jnp.sin(angles)[:, None, :]


def rope_apply(heads_in, cos_tab, sin_tab):
    half_dim = HEAD_DIM // 2
    first_half = heads_in[..., :half_dim]
    second_half = heads_in[..., half_dim:]
    return jnp.concatenate([first_half * cos_tab - second_half * sin_tab, second_half * cos_tab + first_half * sin_tab], axis=-1)


def attend_sequence(triple):
    q_seq, k_seq, v_seq = triple
    scores = jnp.einsum('qhd,khd->hqk', q_seq, k_seq) * (HEAD_DIM ** -0.5)
    causal = jnp.arange(SEQ_LEN)[:, None] >= jnp.arange(SEQ_LEN)[None, :]
    scores = jnp.where(causal[None, :, :], scores, -1e30)
    attn_probs = snap_bf16(jax.nn.softmax(scores, axis=-1))
    return jnp.einsum('hqk,khd->qhd', attn_probs, v_seq)


def block_forward(x_float, w_q, w_k, w_v, w_o, q_norm_w, k_norm_w, post_norm_w):
    tokens = x_float.reshape(-1, D_MODEL)
    head_shape = (BATCH_SIZE, SEQ_LEN, N_HEADS, HEAD_DIM)
    cos_tab, sin_tab = rope_tables()
    q_lin = snap_bf16(jnp.dot(tokens, w_q, preferred_element_type=jnp.float32))
    k_lin = snap_bf16(jnp.dot(tokens, w_k, preferred_element_type=jnp.float32))
    v_lin = snap_bf16(jnp.dot(tokens, w_v, preferred_element_type=jnp.float32))
    q_rot = snap_bf16(rope_apply(rms_norm(q_lin, q_norm_w).reshape(head_shape), cos_tab, sin_tab))
    k_rot = snap_bf16(rope_apply(rms_norm(k_lin, k_norm_w).reshape(head_shape), cos_tab, sin_tab))
    v_heads = v_lin.reshape(head_shape)
    attn_out = lax.map(jax.checkpoint(attend_sequence), (q_rot, k_rot, v_heads))
    attn_tok = snap_bf16(attn_out).reshape(-1, D_MODEL)
    a_lin = snap_bf16(jnp.dot(attn_tok, w_o, preferred_element_type=jnp.float32))
    return x_float + rms_norm(a_lin, post_norm_w).reshape(x_float.shape)


def reference(x, grad_y, w_q, w_k, w_v, w_o, q_norm_w, k_norm_w, post_norm_w):
    y_value, pullback = jax.vjp(block_forward, x.astype(jnp.float32), w_q.astype(jnp.float32), w_k.astype(jnp.float32), w_v.astype(jnp.float32), w_o.astype(jnp.float32), q_norm_w, k_norm_w, post_norm_w)
    all_grads = pullback(grad_y.astype(jnp.float32))
    return (y_value.astype(jnp.bfloat16), all_grads[0].astype(jnp.bfloat16), all_grads[1], all_grads[2], all_grads[3], all_grads[4], all_grads[5], all_grads[6], all_grads[7])
```

```python
import functools

import jax
import jax.numpy as jnp
from jax import lax
from jax.experimental import pallas as pl
from jax.experimental.pallas import tpu as pltpu
from jax.sharding import PartitionSpec as P


HEAD_DIM = 128
RMS_EPSILON = 1e-6
ROPE_THETA = 500000.0
LOG2E = 1.4426950408889634
N_CHUNKS = 2
F32 = jnp.float32
BF16 = jnp.bfloat16
VMEM_BYTES = 58 * 1024 * 1024
ROWS = 16


def rope_tables(seq_len):
    half_dim = HEAD_DIM // 2
    inv_freq = ROPE_THETA ** (-jnp.arange(half_dim, dtype=F32) * (2.0 / HEAD_DIM))
    angles = jnp.arange(seq_len).astype(F32)[:, None] * inv_freq[None, :]
    cos, sin = jnp.cos(angles), jnp.sin(angles)
    return jnp.concatenate([cos, cos], axis=1), jnp.concatenate([-sin, sin], axis=1)


def dot_nn(a, b):
    return lax.dot_general(a, b, (((1,), (0,)), ((), ())), preferred_element_type=F32)


def dot_nt(a, b):
    return lax.dot_general(a, b, (((1,), (1,)), ((), ())), preferred_element_type=F32)


def dot_tn(a, b):
    return lax.dot_general(a, b, (((0,), (0,)), ((), ())), preferred_element_type=F32)


def head_cols(h):
    return pl.ds(pl.multiple_of(h * HEAD_DIM, HEAD_DIM), HEAD_DIM)


def run_heads(n_heads, stages):
    depth = len(stages)

    def step(h, parity, lo, hi):
        for d in reversed(range(depth)):
            if lo <= d <= hi:
                stages[d](h - d, (parity + d) % 2)

    for h in range(depth - 1):
        step(h, h % 2, 0, h)

    def pair(i, carry):
        h = 2 * i + depth - 1
        step(h, (depth - 1) % 2, 0, depth)
        step(h + 1, depth % 2, 0, depth)
        return carry

    n_full = n_heads - (depth - 1)
    lax.fori_loop(0, n_full // 2, pair, 0)
    for h in range(depth - 1 + n_full // 2 * 2, n_heads):
        step(h, h % 2, 0, depth)
    for h in range(n_heads, n_heads + depth - 1):
        step(h, h % 2, h - n_heads + 1, depth)


def pick_halves(side, own, peer):
    mine_first = side == 0
    return jnp.where(mine_first, own, peer), jnp.where(mine_first, peer, own)


def attn_fwd_kernel(side_ref, q0_ref, k0_ref, v_ref, gq_ref, gk_ref, cos_ref, sin_ref,
                    o_ref, qr_ref, kr_ref, iq_ref, ik_ref, s_bufs, p_bufs):
    side = side_ref[0]
    tok_len, width = q0_ref.shape[2], q0_ref.shape[3]
    n_heads = width // HEAD_DIM
    scale = LOG2E * HEAD_DIM ** -0.5
    first, second = side, 1 - side

    def stats(r, carry):
        rows = pl.ds(r * ROWS, ROWS)
        for src, dst in ((q0_ref, iq_ref), (k0_ref, ik_ref)):
            for slot in range(2):
                vals = src[slot, 0, rows, :].astype(F32)
                inv = lax.rsqrt(jnp.mean(vals * vals, axis=-1, keepdims=True) + RMS_EPSILON)
                dst[slot, 0, rows, :] = jnp.broadcast_to(inv, (ROWS, HEAD_DIM))
        return carry

    lax.fori_loop(0, tok_len // ROWS, stats, 0, unroll=4 if tok_len >= 4 * ROWS else 1)

    def scores(h, parity):
        cols = head_cols(h)
        rot = []
        for src, inv, gain, dst in ((q0_ref, iq_ref, gq_ref, qr_ref), (k0_ref, ik_ref, gk_ref, kr_ref)):
            slots = []
            for slot in range(2):
                pos = pl.ds(pl.multiple_of((side if slot == 0 else 1 - side) * tok_len, tok_len), tok_len)
                u = src[slot, 0, :, cols].astype(F32) * inv[slot, 0, :, :] * gain[:, cols]
                slots.append((u * cos_ref[pos, :] + pltpu.roll(u, HEAD_DIM // 2, 1) * sin_ref[pos, :]).astype(BF16))
            lo, hi = pick_halves(side, *slots)
            dst[0, :tok_len, cols] = lo
            dst[0, tok_len:, cols] = hi
            rot += [lo, hi]
        q_lo, q_hi, k_lo, k_hi = rot
        s = s_bufs[parity]
        s[0] = dot_nt(q_lo, k_lo)
        s[1] = dot_nt(q_hi, k_lo)
        s[2] = dot_nt(q_hi, k_hi)

    part = min(64, tok_len)

    def softmax(h, parity):
        s, p = s_bufs[parity], p_bufs[parity]
        for r in range(0, tok_len, part):
            rows = slice(r, r + part)
            keep = (lax.broadcasted_iota(jnp.int32, (part, tok_len), 0) + r >= lax.broadcasted_iota(jnp.int32, (part, tok_len), 1))
            s0 = jnp.where(keep, s[0, rows, :], -1e30)
            p0 = jnp.exp2((s0 - jnp.max(s0, axis=-1, keepdims=True)) * scale)
            p[0, rows, :] = (p0 * (1.0 / jnp.sum(p0, axis=-1, keepdims=True))).astype(BF16)
            s1 = s[1, rows, :]
            s2 = jnp.where(keep, s[2, rows, :], -1e30)
            top = jnp.max(jnp.maximum(s1, s2), axis=-1, keepdims=True)
            p1 = jnp.exp2((s1 - top) * scale)
            p2 = jnp.exp2((s2 - top) * scale)
            rec = 1.0 / jnp.sum(p1 + p2, axis=-1, keepdims=True)
            p[1, rows, :] = (p1 * rec).astype(BF16)
            p[2, rows, :] = (p2 * rec).astype(BF16)

    def mix(h, parity):
        cols = head_cols(h)
        p = p_bufs[parity]
        v_lo, v_hi = v_ref[first, 0, :, cols], v_ref[second, 0, :, cols]
        o_ref[first, 0, :, cols] = dot_nn(p[0], v_lo).astype(BF16)
        o_ref[second, 0, :, cols] = (dot_nn(p[1], v_lo) + dot_nn(p[2], v_hi)).astype(BF16)

    run_heads(n_heads, (scores, softmax, mix))


def attn_fwd(side, q0, k0, v, gain_q, gain_k, cos, sin):
    _, n_seq, tok_len, width = q0.shape
    seq_len = 2 * tok_len
    halves = pl.BlockSpec((2, 1, tok_len, width), lambda j, s: (0, j, 0, 0))
    whole = pl.BlockSpec((1, seq_len, width), lambda j, s: (j, 0, 0))
    inv = pl.BlockSpec((2, 1, tok_len, HEAD_DIM), lambda j, s: (0, j, 0, 0))
    vec = pl.BlockSpec((1, width), lambda j, s: (0, 0))
    tab = pl.BlockSpec((seq_len, HEAD_DIM), lambda j, s: (0, 0))
    n_heads = width // HEAD_DIM
    square = (3, tok_len, tok_len)
    return pl.pallas_call(
        attn_fwd_kernel,
        grid_spec=pltpu.PrefetchScalarGridSpec(
            num_scalar_prefetch=1, grid=(n_seq,),
            in_specs=[halves, halves, halves, vec, vec, tab, tab],
            out_specs=[halves, whole, whole, inv, inv],
            scratch_shapes=[[pltpu.VMEM(square, F32)] * 2, [pltpu.VMEM(square, BF16)] * 2]),
        out_shape=[jax.ShapeDtypeStruct(q0.shape, BF16)]
        + [jax.ShapeDtypeStruct((n_seq, seq_len, width), BF16)] * 2
        + [jax.ShapeDtypeStruct((2, n_seq, tok_len, HEAD_DIM), F32)] * 2,
        compiler_params=pltpu.CompilerParams(vmem_limit_bytes=VMEM_BYTES),
        cost_estimate=pl.CostEstimate(
            flops=n_seq * n_heads * 2 * 4 * tok_len * tok_len * 3 * HEAD_DIM * 2,
            bytes_accessed=n_seq * seq_len * width * 12, transcendentals=n_seq * n_heads * 3 * tok_len * tok_len),
        name="attn_fwd",
    )(side, q0, k0, v, gain_q, gain_k, cos, sin)


def attn_bwd_kernel(side_ref, qr_ref, kr_ref, v_ref, do_ref, q0_ref, k0_ref, iq_ref, ik_ref, gq_ref, gk_ref, cos_ref, sin_ref,
                    dq_ref, dk_ref, dv_ref, gqp_ref, gkp_ref,
                    acc_q, acc_k, proj_q, proj_k, s_bufs, d_bufs, p_bufs, ds_bufs):
    side = side_ref[0]
    tok_len, width = q0_ref.shape[2], q0_ref.shape[3]
    n_heads = width // HEAD_DIM
    scale = LOG2E * HEAD_DIM ** -0.5
    back_scale = HEAD_DIM ** -0.5
    first, second = side, 1 - side
    lo, hi = slice(0, tok_len), slice(tok_len, 2 * tok_len)

    @pl.when(pl.program_id(0) == 0)
    def _():
        gqp_ref[...] = jnp.zeros_like(gqp_ref)
        gkp_ref[...] = jnp.zeros_like(gkp_ref)

    proj_q[...] = jnp.zeros_like(proj_q)
    proj_k[...] = jnp.zeros_like(proj_k)

    def scores(h, parity):
        cols = head_cols(h)
        k_lo, k_hi = kr_ref[0, lo, cols], kr_ref[0, hi, cols]
        q_lo, q_hi = qr_ref[0, lo, cols], qr_ref[0, hi, cols]
        v_lo, v_hi = v_ref[first, 0, :, cols], v_ref[second, 0, :, cols]
        do_lo, do_hi = do_ref[first, 0, :, cols], do_ref[second, 0, :, cols]
        s, d = s_bufs[parity], d_bufs[parity]
        s[0] = dot_nt(k_lo, q_lo)
        s[1] = dot_nt(k_lo, q_hi)
        s[2] = dot_nt(k_hi, q_hi)
        d[0] = dot_nt(v_lo, do_lo)
        d[1] = dot_nt(v_lo, do_hi)
        d[2] = dot_nt(v_hi, do_hi)

    part = min(128, tok_len)

    def softmax(h, parity):
        s, d, p, ds = s_bufs[parity], d_bufs[parity], p_bufs[parity], ds_bufs[parity]
        for c in range(0, tok_len, part):
            cols = slice(c, c + part)
            keep = (lax.broadcasted_iota(jnp.int32, (tok_len, part), 0) <= lax.broadcasted_iota(jnp.int32, (tok_len, part), 1) + c)
            for blocks in ((0,), (1, 2)):
                raw = [s[b, :, cols] for b in blocks]
                raw[-1] = jnp.where(keep, raw[-1], -1e30)
                top = functools.reduce(jnp.maximum, [jnp.max(r, axis=0, keepdims=True) for r in raw])
                e = [jnp.exp2((r - top) * scale) for r in raw]
                rec = 1.0 / sum(jnp.sum(r, axis=0, keepdims=True) for r in e)
                delta = sum(jnp.sum(r * d[b, :, cols], axis=0, keepdims=True) for r, b in zip(e, blocks)) * rec
                for r, b in zip(e, blocks):
                    prob = r * rec
                    p[b, :, cols] = prob.astype(BF16)
                    ds[b, :, cols] = (prob * (d[b, :, cols] - delta)).astype(BF16)

    def grads(h, parity):
        cols = head_cols(h)
        k_lo, k_hi = kr_ref[0, lo, cols], kr_ref[0, hi, cols]
        q_lo, q_hi = qr_ref[0, lo, cols], qr_ref[0, hi, cols]
        do_lo, do_hi = do_ref[first, 0, :, cols], do_ref[second, 0, :, cols]
        p, ds = p_bufs[parity], ds_bufs[parity]
        dv_ref[first, 0, :, cols] = (dot_nn(p[0], do_lo) + dot_nn(p[1], do_hi)).astype(BF16)
        dv_ref[second, 0, :, cols] = dot_nn(p[2], do_hi).astype(BF16)
        dq_lo = dot_tn(ds[0], k_lo)
        dq_hi = dot_tn(ds[1], k_lo) + dot_tn(ds[2], k_hi)
        dk_lo = dot_nn(ds[0], q_lo) + dot_nn(ds[1], q_hi)
        dk_hi = dot_nn(ds[2], q_hi)
        for pair, src, inv, gain, acc, proj, part_ref in (((dq_lo, dq_hi), q0_ref, iq_ref, gq_ref, acc_q, proj_q, gqp_ref),
                                                          ((dk_lo, dk_hi), k0_ref, ik_ref, gk_ref, acc_k, proj_k, gkp_ref)):
            total = jnp.zeros((8, HEAD_DIM), F32)
            for g, rows, slot in zip(pair, (lo, hi), (first, second)):
                g = g * back_scale
                g = g * cos_ref[rows, :] - pltpu.roll(g, HEAD_DIM // 2, 1) * sin_ref[rows, :]
                hat = src[slot, 0, :, cols].astype(F32) * inv[slot, 0, :, :]
                prod = g * hat
                total += jnp.sum(prod.reshape(tok_len // 8, 8, HEAD_DIM), axis=0)
                proj[rows, :] += prod * gain[:, cols]
                acc[rows, cols] = g * gain[:, cols]
            part_ref[:, cols] += total

    run_heads(n_heads, (scores, softmax, grads))

    for proj, inv in ((proj_q, iq_ref), (proj_k, ik_ref)):
        for rows, slot in ((lo, first), (hi, second)):
            i = inv[slot, 0, :, :]
            proj[rows, :] = jnp.sum(proj[rows, :], axis=-1, keepdims=True) * (1.0 / width) * i * i

    def finish(r, carry):
        rows = pl.ds(r * ROWS, ROWS)
        for acc, src, inv, proj, dst in ((acc_q, q0_ref, iq_ref, proj_q, dq_ref), (acc_k, k0_ref, ik_ref, proj_k, dk_ref)):
            for slot in range(2):
                pos = pl.ds(pl.multiple_of((side if slot == 0 else 1 - side) * tok_len + r * ROWS, ROWS), ROWS)
                i, c = inv[slot, 0, rows, :], proj[pos, :]
                for h in range(n_heads):
                    cols = slice(h * HEAD_DIM, (h + 1) * HEAD_DIM)
                    dst[slot, 0, rows, cols] = (acc[pos, cols] * i - src[slot, 0, rows, cols].astype(F32) * c).astype(BF16)
        return carry

    lax.fori_loop(0, tok_len // ROWS, finish, 0)


def attn_bwd(side, chunk, q_rot, k_rot, v, d_out, q0, k0, inv_q, inv_k, gain_q, gain_k, cos, sin):
    _, n_seq, tok_len, width = d_out.shape
    seq_len = 2 * tok_len
    first = chunk * n_seq
    halves = pl.BlockSpec((2, 1, tok_len, width), lambda j, s: (0, first + j, 0, 0))
    part_halves = pl.BlockSpec((2, 1, tok_len, width), lambda j, s: (0, j, 0, 0))
    whole = pl.BlockSpec((1, seq_len, width), lambda j, s: (first + j, 0, 0))
    inv = pl.BlockSpec((2, 1, tok_len, HEAD_DIM), lambda j, s: (0, first + j, 0, 0))
    vec = pl.BlockSpec((1, width), lambda j, s: (0, 0))
    part = pl.BlockSpec((8, width), lambda j, s: (0, 0))
    tab = pl.BlockSpec((seq_len, HEAD_DIM), lambda j, s: (0, 0))
    n_heads = width // HEAD_DIM
    square = (3, tok_len, tok_len)
    return pl.pallas_call(
        attn_bwd_kernel,
        grid_spec=pltpu.PrefetchScalarGridSpec(
            num_scalar_prefetch=1, grid=(n_seq,),
            in_specs=[whole, whole, halves, part_halves, halves, halves, inv, inv, vec, vec, tab, tab],
            out_specs=[part_halves, part_halves, part_halves, part, part],
            scratch_shapes=[pltpu.VMEM((seq_len, width), F32)] * 2 + [pltpu.VMEM((seq_len, HEAD_DIM), F32)] * 2
            + [[pltpu.VMEM(square, F32)] * 2] * 2 + [[pltpu.VMEM(square, BF16)] * 2] * 2),
        out_shape=[jax.ShapeDtypeStruct(d_out.shape, BF16)] * 3 + [jax.ShapeDtypeStruct((8, width), F32)] * 2,
        compiler_params=pltpu.CompilerParams(vmem_limit_bytes=VMEM_BYTES),
        cost_estimate=pl.CostEstimate(
            flops=n_seq * n_heads * 2 * 10 * tok_len * tok_len * 3 * HEAD_DIM * 2,
            bytes_accessed=n_seq * seq_len * width * 18, transcendentals=n_seq * n_heads * 3 * tok_len * tok_len),
        name="attn_bwd",
    )(side, q_rot, k_rot, v, d_out, q0, k0, inv_q, inv_k, gain_q, gain_k, cos, sin)


def tile_of(n, most):
    return most if n % most == 0 else n


def matmul_kernel(side_ref, a_ref, b_ref, *rest):
    rest[-1][...] = dot_nn(a_ref[...], b_ref[...]).astype(BF16)


def matmul(side, a, b, out_rows, out_block, n_blocks, own=False, into=None):
    depth, width = b.shape
    rows = out_rows // 4
    tile = tile_of(width, 512)
    row_block = (lambda i, s: s[0] * n_blocks + i) if own else (lambda i, s: i)
    specs = [pl.BlockSpec((rows, depth), lambda i, j, s: (row_block(i, s), 0)), pl.BlockSpec((depth, tile), lambda i, j, s: (0, j))]
    args = [side, a, b]
    if into is not None:
        specs.append(pl.BlockSpec(memory_space=pl.ANY))
        args.append(into)
    return pl.pallas_call(
        matmul_kernel,
        grid_spec=pltpu.PrefetchScalarGridSpec(
            num_scalar_prefetch=1, grid=(n_blocks, width // tile), in_specs=specs,
            out_specs=pl.BlockSpec((rows, tile), lambda i, j, s: (out_block + i, j))),
        out_shape=jax.ShapeDtypeStruct((out_rows, width), BF16),
        input_output_aliases={} if into is None else {3: 0},
        compiler_params=pltpu.CompilerParams(vmem_limit_bytes=VMEM_BYTES),
        cost_estimate=pl.CostEstimate(flops=2 * n_blocks * rows * depth * width, transcendentals=0,
                                      bytes_accessed=2 * (2 * n_blocks * rows * width + depth * width)),
        name="matmul",
    )(*args)


def matmul_nt_kernel(a_ref, b_ref, o_ref):
    o_ref[...] = dot_nt(a_ref[...], b_ref[...]).astype(BF16)


def matmul_nt(a, b):
    n_rows, depth = a.shape
    width = b.shape[0]
    rows, tile = n_rows // 2, tile_of(width, 512)
    return pl.pallas_call(
        matmul_nt_kernel, grid=(2, width // tile),
        in_specs=[pl.BlockSpec((rows, depth), lambda i, j: (i, 0)), pl.BlockSpec((tile, depth), lambda i, j: (j, 0))],
        out_specs=pl.BlockSpec((rows, tile), lambda i, j: (i, j)),
        out_shape=jax.ShapeDtypeStruct((n_rows, width), BF16),
        compiler_params=pltpu.CompilerParams(vmem_limit_bytes=VMEM_BYTES),
        cost_estimate=pl.CostEstimate(flops=2 * n_rows * depth * width, transcendentals=0,
                                      bytes_accessed=2 * (2 * n_rows * width + depth * width)),
        name="matmul_nt",
    )(a, b)


def wgrad_kernel(side_ref, *refs):
    *lhs, d0_ref, d1_ref, o_ref = refs
    part = d0_ref.shape[0] // 2
    if len(lhs) == 1:
        blocks = [lhs[0][i * part:(i + 1) * part, :] for i in range(4)]
    else:
        blocks = [lhs[0][:part, :], lhs[0][part:, :], lhs[1][...], lhs[2][...]]
    o_ref[...] = (dot_tn(blocks[0], d0_ref[:part, :]) + dot_tn(blocks[1], d1_ref[:part, :])
                  + dot_tn(blocks[2], d0_ref[part:, :]) + dot_tn(blocks[3], d1_ref[part:, :]))


def wgrad(side, lhs, d0, d1):
    n_rows = d0.shape[0]
    width = d0.shape[1]
    tall, wide = tile_of(width, 1024), tile_of(width, 512)
    if len(lhs) == 1:
        lhs_specs = [pl.BlockSpec((2 * n_rows, tall), lambda i, j, s: (0, i))]
    else:
        lhs_specs = [pl.BlockSpec((n_rows, tall), lambda i, j, s: (s[0], i))]
        lhs_specs += [pl.BlockSpec((n_rows // 2, tall), lambda i, j, s: (0, i))] * 2
    return pl.pallas_call(
        wgrad_kernel,
        grid_spec=pltpu.PrefetchScalarGridSpec(
            num_scalar_prefetch=1, grid=(width // tall, width // wide),
            in_specs=lhs_specs + [pl.BlockSpec((n_rows, wide), lambda i, j, s: (0, j))] * 2,
            out_specs=pl.BlockSpec((tall, wide), lambda i, j, s: (i, j))),
        out_shape=jax.ShapeDtypeStruct((width, width), F32),
        compiler_params=pltpu.CompilerParams(vmem_limit_bytes=VMEM_BYTES),
        cost_estimate=pl.CostEstimate(flops=4 * n_rows * width * width, transcendentals=0, bytes_accessed=12 * n_rows * width),
        name="wgrad",
    )(side, *lhs, d0, d1)


def grad_x_kernel(side_ref, dq_ref, dk_ref, dv_ref, wq_ref, wk_ref, wv_ref, gy_ref, *rest):
    total = dot_nt(dq_ref[...], wq_ref[...]) + dot_nt(dk_ref[...], wk_ref[...]) + dot_nt(dv_ref[...], wv_ref[...])
    rest[-1][...] = (total + gy_ref[...].astype(F32)).astype(BF16)


def grad_x_rows(side, chunk, slot, d, weights, gy, out_rows, into=None):
    width = d[0].shape[1]
    n_rows = d[0].shape[0] // 2
    rows, tile = tile_of(n_rows, 512), tile_of(width, 512)
    steps = n_rows // rows
    row = pl.BlockSpec((rows, width), lambda i, j, s: (slot * steps + i, 0))
    weight = pl.BlockSpec((tile, width), lambda i, j, s: (j, 0))
    place = (lambda i, s: (s[0] * N_CHUNKS + chunk) * steps + i) if slot == 0 else (lambda i, s: i)
    out = pl.BlockSpec((rows, tile), lambda i, j, s: (place(i, s), j))
    specs, args = [row] * 3 + [weight] * 3 + [out], [side, *d, *weights, gy]
    if into is not None:
        specs.append(pl.BlockSpec(memory_space=pl.ANY))
        args.append(into)
    return pl.pallas_call(
        grad_x_kernel,
        grid_spec=pltpu.PrefetchScalarGridSpec(
            num_scalar_prefetch=1, grid=(steps, width // tile), in_specs=specs, out_specs=out),
        out_shape=jax.ShapeDtypeStruct((out_rows, width), BF16),
        input_output_aliases={} if into is None else {8: 0},
        compiler_params=pltpu.CompilerParams(vmem_limit_bytes=VMEM_BYTES),
        cost_estimate=pl.CostEstimate(flops=6 * n_rows * width * width, transcendentals=0,
                                      bytes_accessed=10 * n_rows * width + 6 * width * width),
        name="grad_x",
    )(*args)


def post_kernel(side_ref, a_ref, x_own_ref, x_peer_ref, gy_own_ref, gy_peer_ref, gain_ref, *rest):
    y_own_ref, y_peer_ref, ga_ref, part_ref = rest[-4:]
    step, half = pl.program_id(0), pl.num_programs(0) // 2

    @pl.when(step == 0)
    def _():
        part_ref[...] = jnp.zeros_like(part_ref)

    def run(x_ref, gy_ref, y_ref):
        def rows_step(r, carry):
            rows = pl.ds(r * ROWS, ROWS)
            a = a_ref[rows, :].astype(F32)
            inv = lax.rsqrt(jnp.mean(a * a, axis=-1, keepdims=True) + RMS_EPSILON)
            hat = a * inv
            gain = gain_ref[...]
            y_ref[rows, :] = (x_ref[rows, :].astype(F32) + hat * gain).astype(BF16)
            gy = gy_ref[rows, :].astype(F32)
            prod = gy * hat
            part_ref[...] += prod[:8] + prod[8:]
            proj = jnp.mean(prod * gain, axis=-1, keepdims=True)
            ga_ref[rows, :] = (inv * (gy * gain - hat * proj)).astype(BF16)
            return carry

        lax.fori_loop(0, a_ref.shape[0] // ROWS, rows_step, 0, unroll=4)

    @pl.when(step < half)
    def _():
        run(x_peer_ref, gy_peer_ref, y_peer_ref)

    @pl.when(step >= half)
    def _():
        run(x_own_ref, gy_own_ref, y_own_ref)


def post_norm(side, chunk, a, x, x_peer, gy, gy_peer, gain, into=None):
    n_peer, width = x_peer.shape
    block = min(256, n_peer)
    half = n_peer // block
    all_half = N_CHUNKS * half

    def peer(i, s):
        return jnp.minimum(i, half - 1), 0

    def own(i, s):
        return (s[0] * N_CHUNKS + chunk) * half + jnp.maximum(i - half, 0), 0

    def a_rows(i, s):
        return jnp.where(i < half, all_half + chunk * half + i, chunk * half + i - half), 0

    def ga_rows(i, s):
        return jnp.where(i < half, half + i, i - half), 0

    def spec(index):
        return pl.BlockSpec((block, width), index)

    specs = [spec(a_rows), spec(own), spec(peer), spec(own), spec(peer), pl.BlockSpec((1, width), lambda i, s: (0, 0))]
    args = [side, a, x, x_peer, gy, gy_peer, gain]
    if into is not None:
        specs.append(pl.BlockSpec(memory_space=pl.ANY))
        args.append(into)
    return pl.pallas_call(
        post_kernel,
        grid_spec=pltpu.PrefetchScalarGridSpec(
            num_scalar_prefetch=1, grid=(2 * half,), in_specs=specs,
            out_specs=[spec(own), spec(peer), spec(ga_rows), pl.BlockSpec((8, width), lambda i, s: (0, 0))]),
        out_shape=[jax.ShapeDtypeStruct(x.shape, BF16), jax.ShapeDtypeStruct(x_peer.shape, BF16),
                   jax.ShapeDtypeStruct((2 * n_peer, width), BF16), jax.ShapeDtypeStruct((8, width), F32)],
        input_output_aliases={} if into is None else {7: 0},
        compiler_params=pltpu.CompilerParams(vmem_limit_bytes=VMEM_BYTES),
        cost_estimate=pl.CostEstimate(flops=2 * n_peer * width * 2000, bytes_accessed=n_peer * width * 20, transcendentals=n_peer),
        name="post_norm",
    )(*args)


def solution(mesh):
    tok_spec = P('fsdp', 'sp', None)
    row_spec = P('fsdp', None)
    vec_spec = P('fsdp')
    swap = [(0, 1), (1, 0)]

    def body(x, grad_y, wq_rows, wk_rows, wv_rows, wo_rows, gq_rows, gk_rows, gpost_rows):
        n_batch, tok_len, width = x.shape
        n_own = n_batch // 2
        n_seq = n_own // N_CHUNKS
        n_part = n_seq * tok_len
        all_rows = n_batch * tok_len
        chunks = range(N_CHUNKS)
        my_side = lax.axis_index('sp')
        side = my_side.astype(jnp.int32).reshape(1)
        peer_start = (1 - my_side) * n_own

        def send(part):
            return lax.ppermute(part, 'sp', swap)

        def fetch(array):
            parts = [lax.dynamic_slice_in_dim(array, peer_start + c * n_seq, n_seq) for c in chunks]
            return [send(parts[c]).reshape(n_part, width) for c in chunks]

        x_peer = fetch(x)
        gy_peer = fetch(grad_y)
        x_flat, gy_flat = x.reshape(all_rows, width), grad_y.reshape(all_rows, width)

        w_q, w_k, w_v, w_o = (lax.all_gather(w, 'fsdp', axis=0, tiled=True) for w in (wq_rows, wk_rows, wv_rows, wo_rows))
        gains = lax.all_gather(jnp.stack([gq_rows, gk_rows, gpost_rows]), 'fsdp', axis=1, tiled=True)
        gain_q, gain_k, gain_post = gains[0:1], gains[1:2], gains[2:3]
        cos, sin = rope_tables(2 * tok_len)

        def halves(a):
            return a.reshape(2, a.shape[0] // (2 * tok_len), tok_len, width)

        def flat(a):
            return a.reshape(-1, width)

        def project(w):
            out = matmul(side, x_flat, w, all_rows, 0, 2, own=True)
            for c in chunks:
                out = matmul(side, x_peer[c], w, all_rows, 2 + c, 1, into=out)
            return halves(out)

        q0, k0, v = project(w_q), project(w_k), project(w_v)
        o, q_rot, k_rot, inv_q, inv_k = attn_fwd(side, q0, k0, v, gain_q, gain_k, cos, sin)
        a_lin = matmul(side, flat(o), w_o, all_rows, 0, 4)

        y, ga, y_peer, post_parts, grads = None, [], [], [], []
        for c in chunks:
            y, y_send, ga_c, part = post_norm(side, c, a_lin, x_flat, x_peer[c], gy_flat, gy_peer[c], gain_post, into=y)
            ga.append(ga_c)
            post_parts.append(part)
            y_peer.append(send(y_send.reshape(n_seq, tok_len, width)))
        y = y.reshape(x.shape)
        for c in chunks:
            y = lax.dynamic_update_slice_in_dim(y, y_peer[c], peer_start + c * n_seq, 0)

        for c in chunks:
            d_o = halves(matmul_nt(ga[c], w_o))
            grads.append(attn_bwd(side, c, q_rot, k_rot, v, d_o, q0, k0, inv_q, inv_k, gain_q, gain_k, cos, sin))

        def weight_grad(lhs, d):
            part = wgrad(side, lhs, *d)
            rows = lax.psum_scatter(part, 'fsdp', scatter_dimension=0, tiled=True)
            return rows + send(rows)

        d_q, d_k, d_v = ([flat(g[i]) for g in grads] for i in range(3))
        g_wo = weight_grad((flat(o),), ga)
        g_wv = weight_grad((x_flat, *x_peer), d_v)
        g_wk = weight_grad((x_flat, *x_peer), d_k)
        g_wq = weight_grad((x_flat, *x_peer), d_q)

        gx_peer, grad_x = [], None
        for c in chunks:
            gx = grad_x_rows(side, c, 1, (d_q[c], d_k[c], d_v[c]), (w_q, w_k, w_v), gy_peer[c], n_part)
            gx_peer.append(send(gx.reshape(n_seq, tok_len, width)))
        for c in chunks:
            grad_x = grad_x_rows(side, c, 0, (d_q[c], d_k[c], d_v[c]), (w_q, w_k, w_v), gy_flat, all_rows, into=grad_x)
        grad_x = grad_x.reshape(x.shape)
        for c in chunks:
            grad_x = lax.dynamic_update_slice_in_dim(grad_x, gx_peer[c], peer_start + c * n_seq, 0)

        parts = jnp.stack([sum(g[3] for g in grads).sum(0), sum(g[4] for g in grads).sum(0), sum(post_parts).sum(0)])
        for axis, flip in (("sp", 1), ("fsdp", 1), ("fsdp", 2), ("fsdp", 4)):
            parts = parts + lax.ppermute(parts, axis, [(d, d ^ flip) for d in range(mesh.shape[axis])])
        n_vec = gq_rows.shape[0]
        g_vec = lax.dynamic_slice_in_dim(parts, lax.axis_index('fsdp') * n_vec, n_vec, axis=1)
        return y, grad_x, g_wq, g_wk, g_wv, g_wo, g_vec[0], g_vec[1], g_vec[2]

    specs = (tok_spec, tok_spec, row_spec, row_spec, row_spec, row_spec, vec_spec, vec_spec, vec_spec)
    return jax.shard_map(body, mesh=mesh, in_specs=specs, out_specs=specs, check_vma=False)
```

```python
import functools

import jax
import jax.numpy as jnp
from jax import lax
from jax.experimental import pallas as pl
from jax.experimental.pallas import tpu as pltpu
from jax.sharding import PartitionSpec as P


HEAD_DIM = 128
RMS_EPSILON = 1e-6
ROPE_THETA = 500000.0
LOG2E = 1.4426950408889634
N_CHUNKS = 2
F32 = jnp.float32
BF16 = jnp.bfloat16
VMEM_BYTES = 58 * 1024 * 1024
ROWS = 16


def rope_tables(seq_len):
    half_dim = HEAD_DIM // 2
    inv_freq = ROPE_THETA ** (-jnp.arange(half_dim, dtype=F32) * (2.0 / HEAD_DIM))
    angles = jnp.arange(seq_len).astype(F32)[:, None] * inv_freq[None, :]
    cos, sin = jnp.cos(angles), jnp.sin(angles)
    return jnp.concatenate([cos, cos], axis=1), jnp.concatenate([-sin, sin], axis=1)


def dot_nn(a, b):
    return lax.dot_general(a, b, (((1,), (0,)), ((), ())), preferred_element_type=F32)


def dot_nt(a, b):
    return lax.dot_general(a, b, (((1,), (1,)), ((), ())), preferred_element_type=F32)


def dot_tn(a, b):
    return lax.dot_general(a, b, (((0,), (0,)), ((), ())), preferred_element_type=F32)


def head_cols(h):
    return pl.ds(pl.multiple_of(h * HEAD_DIM, HEAD_DIM), HEAD_DIM)


def run_heads(n_heads, stages):
    depth = len(stages)

    def step(h, parity, lo, hi):
        for d in reversed(range(depth)):
            if lo <= d <= hi:
                stages[d](h - d, (parity + d) % 2)

    for h in range(depth - 1):
        step(h, h % 2, 0, h)

    def pair(i, carry):
        h = 2 * i + depth - 1
        step(h, (depth - 1) % 2, 0, depth)
        step(h + 1, depth % 2, 0, depth)
        return carry

    n_full = n_heads - (depth - 1)
    lax.fori_loop(0, n_full // 2, pair, 0)
    for h in range(depth - 1 + n_full // 2 * 2, n_heads):
        step(h, h % 2, 0, depth)
    for h in range(n_heads, n_heads + depth - 1):
        step(h, h % 2, h - n_heads + 1, depth)


def seen_pieces(half, c, part, tok_len):
    diagonal = 2 * half
    pieces = [(1, 0, tok_len)] if half else []
    if c:
        pieces.append((diagonal, 0, c))
    return pieces + [(diagonal, c, c + part)]


def store_scores(out, a_lo, a_hi, b_lo, b_hi, part):
    for block, a, b in ((0, a_lo, b_lo), (2, a_hi, b_hi)):
        for c in range(0, a.shape[0], part):
            out[block, c:c + part, c:] = dot_nt(a[c:c + part], b[c:])
    out[1] = dot_nt(a_lo, b_hi)


def clear_unseen(bufs, part):
    @pl.when(pl.program_id(0) == 0)
    def _():
        for buf in bufs:
            for block in (0, 2):
                for c in range(part, buf.shape[1], part):
                    buf[block, c:c + part, :c] = jnp.zeros((part, c), buf.dtype)


def pick_halves(side, own, peer):
    mine_first = side == 0
    return jnp.where(mine_first, own, peer), jnp.where(mine_first, peer, own)


def attn_fwd_kernel(side_ref, q0_ref, k0_ref, v_ref, gq_ref, gk_ref, cos_ref, sin_ref,
                    o_ref, qr_ref, kr_ref, iq_ref, ik_ref, lse_ref, s_bufs, p_bufs):
    side = side_ref[0]
    tok_len, width = q0_ref.shape[2], q0_ref.shape[3]
    n_heads = width // HEAD_DIM
    scale = LOG2E * HEAD_DIM ** -0.5
    first, second = side, 1 - side

    def stats(r, carry):
        rows = pl.ds(r * ROWS, ROWS)
        for src, dst in ((q0_ref, iq_ref), (k0_ref, ik_ref)):
            for slot in range(2):
                vals = src[slot, 0, rows, :].astype(F32)
                inv = lax.rsqrt(jnp.mean(vals * vals, axis=-1, keepdims=True) + RMS_EPSILON)
                dst[slot, 0, rows, :] = jnp.broadcast_to(inv, (ROWS, HEAD_DIM))
        return carry

    lax.fori_loop(0, tok_len // ROWS, stats, 0, unroll=4 if tok_len >= 4 * ROWS else 1)
    part = min(128, tok_len)
    keep = (lax.broadcasted_iota(jnp.int32, (part, part), 0) <= lax.broadcasted_iota(jnp.int32, (part, part), 1))
    clear_unseen(p_bufs, part)

    def scores(h, parity):
        cols = head_cols(h)
        rot = []
        for src, inv, gain, dst in ((q0_ref, iq_ref, gq_ref, qr_ref), (k0_ref, ik_ref, gk_ref, kr_ref)):
            slots = []
            for slot in range(2):
                pos = pl.ds(pl.multiple_of((side if slot == 0 else 1 - side) * tok_len, tok_len), tok_len)
                u = src[slot, 0, :, cols].astype(F32) * inv[slot, 0, :, :] * gain[:, cols]
                slots.append((u * cos_ref[pos, :] + pltpu.roll(u, HEAD_DIM // 2, 1) * sin_ref[pos, :]).astype(BF16))
            lo, hi = pick_halves(side, *slots)
            dst[0, :tok_len, cols] = lo
            dst[0, tok_len:, cols] = hi
            rot += [lo, hi]
        q_lo, q_hi, k_lo, k_hi = rot
        store_scores(s_bufs[parity], k_lo, k_hi, q_lo, q_hi, part)

    def softmax(h, parity):
        s, p = s_bufs[parity], p_bufs[parity]
        for c in range(0, tok_len, part):
            cols = slice(c, c + part)
            for half in range(2):
                pieces = seen_pieces(half, c, part, tok_len)
                raw = [s[b, i:j, cols] for b, i, j in pieces]
                raw[-1] = jnp.where(keep, raw[-1], -1e30)
                top = functools.reduce(jnp.maximum, [jnp.max(r, axis=0, keepdims=True) for r in raw])
                prob = [jnp.exp2((r - top) * scale) for r in raw]
                total = sum(jnp.sum(r, axis=0, keepdims=True) for r in prob)
                rec = 1.0 / total
                for r, (b, i, j) in zip(prob, pieces):
                    p[b, i:j, cols] = (r * rec).astype(BF16)
                lse = top * scale + jnp.log2(total)
                lse_ref[0, h, :, half * tok_len + c:half * tok_len + c + part] = jnp.broadcast_to(lse, (8, part))

    def mix(h, parity):
        cols = head_cols(h)
        p = p_bufs[parity]
        v_lo, v_hi = v_ref[first, 0, :, cols], v_ref[second, 0, :, cols]
        o_ref[first, 0, :, cols] = dot_tn(p[0], v_lo).astype(BF16)
        o_ref[second, 0, :, cols] = (dot_tn(p[1], v_lo) + dot_tn(p[2], v_hi)).astype(BF16)

    run_heads(n_heads, (scores, softmax, mix))


def attn_fwd(side, q0, k0, v, gain_q, gain_k, cos, sin):
    _, n_seq, tok_len, width = q0.shape
    seq_len = 2 * tok_len
    halves = pl.BlockSpec((2, 1, tok_len, width), lambda j, s: (0, j, 0, 0))
    whole = pl.BlockSpec((1, seq_len, width), lambda j, s: (j, 0, 0))
    inv = pl.BlockSpec((2, 1, tok_len, HEAD_DIM), lambda j, s: (0, j, 0, 0))
    vec = pl.BlockSpec((1, width), lambda j, s: (0, 0))
    tab = pl.BlockSpec((seq_len, HEAD_DIM), lambda j, s: (0, 0))
    n_heads = width // HEAD_DIM
    square = (3, tok_len, tok_len)
    return pl.pallas_call(
        attn_fwd_kernel,
        grid_spec=pltpu.PrefetchScalarGridSpec(
            num_scalar_prefetch=1, grid=(n_seq,),
            in_specs=[halves, halves, halves, vec, vec, tab, tab],
            out_specs=[halves, whole, whole, inv, inv, pl.BlockSpec((1, n_heads, 8, seq_len), lambda j, s: (j, 0, 0, 0))],
            scratch_shapes=[[pltpu.VMEM(square, F32)] * 2, [pltpu.VMEM(square, BF16)] * 2]),
        out_shape=[jax.ShapeDtypeStruct(q0.shape, BF16)]
        + [jax.ShapeDtypeStruct((n_seq, seq_len, width), BF16)] * 2
        + [jax.ShapeDtypeStruct((2, n_seq, tok_len, HEAD_DIM), F32)] * 2 + [jax.ShapeDtypeStruct((n_seq, n_heads, 8, seq_len), F32)],
        compiler_params=pltpu.CompilerParams(vmem_limit_bytes=VMEM_BYTES),
        cost_estimate=pl.CostEstimate(
            flops=n_seq * n_heads * 2 * 4 * tok_len * tok_len * 3 * HEAD_DIM * 2,
            bytes_accessed=n_seq * seq_len * width * 12, transcendentals=n_seq * n_heads * 3 * tok_len * tok_len),
        name="attn_fwd",
    )(side, q0, k0, v, gain_q, gain_k, cos, sin)


def attn_bwd_kernel(side_ref, qr_ref, kr_ref, v_ref, do_ref, q0_ref, k0_ref, iq_ref, ik_ref, lse_ref, gq_ref, gk_ref, cos_ref, sin_ref,
                    dq_ref, dk_ref, dv_ref, gqp_ref, gkp_ref,
                    acc_q, acc_k, proj_q, proj_k, s_bufs, d_bufs, p_bufs, ds_bufs):
    side = side_ref[0]
    tok_len, width = q0_ref.shape[2], q0_ref.shape[3]
    n_heads = width // HEAD_DIM
    scale = LOG2E * HEAD_DIM ** -0.5
    first, second = side, 1 - side
    lo, hi = slice(0, tok_len), slice(tok_len, 2 * tok_len)

    @pl.when(pl.program_id(0) == 0)
    def _():
        gqp_ref[...] = jnp.zeros_like(gqp_ref)
        gkp_ref[...] = jnp.zeros_like(gkp_ref)

    part = min(128, tok_len)
    keep = (lax.broadcasted_iota(jnp.int32, (part, part), 0) <= lax.broadcasted_iota(jnp.int32, (part, part), 1))
    clear_unseen((*p_bufs, *ds_bufs), part)
    proj_q[...] = jnp.zeros_like(proj_q)
    proj_k[...] = jnp.zeros_like(proj_k)

    def scores(h, parity):
        cols = head_cols(h)
        k_lo, k_hi = kr_ref[0, lo, cols], kr_ref[0, hi, cols]
        q_lo, q_hi = qr_ref[0, lo, cols], qr_ref[0, hi, cols]
        v_lo, v_hi = v_ref[first, 0, :, cols], v_ref[second, 0, :, cols]
        do_lo, do_hi = do_ref[first, 0, :, cols], do_ref[second, 0, :, cols]
        store_scores(s_bufs[parity], k_lo, k_hi, q_lo, q_hi, part)
        store_scores(d_bufs[parity], v_lo, v_hi, do_lo, do_hi, part)

    def softmax(h, parity):
        s, d, p, ds = s_bufs[parity], d_bufs[parity], p_bufs[parity], ds_bufs[parity]
        for c in range(0, tok_len, part):
            cols = slice(c, c + part)
            for half in range(2):
                pieces = seen_pieces(half, c, part, tok_len)
                lse = lse_ref[0, h, 0:1, half * tok_len + c:half * tok_len + c + part]
                prob = [jnp.exp2(s[b, i:j, cols] * scale - lse) for b, i, j in pieces]
                prob[-1] = jnp.where(keep, prob[-1], 0.0)
                delta = sum(jnp.sum(r * d[b, i:j, cols], axis=0, keepdims=True) for r, (b, i, j) in zip(prob, pieces))
                for r, (b, i, j) in zip(prob, pieces):
                    p[b, i:j, cols] = r.astype(BF16)
                    ds[b, i:j, cols] = (r * (d[b, i:j, cols] - delta)).astype(BF16)

    def grads(h, parity):
        cols = head_cols(h)
        k_lo, k_hi = kr_ref[0, lo, cols], kr_ref[0, hi, cols]
        q_lo, q_hi = qr_ref[0, lo, cols], qr_ref[0, hi, cols]
        do_lo, do_hi = do_ref[first, 0, :, cols], do_ref[second, 0, :, cols]
        p, ds = p_bufs[parity], ds_bufs[parity]
        dv_ref[first, 0, :, cols] = (dot_nn(p[0], do_lo) + dot_nn(p[1], do_hi)).astype(BF16)
        dv_ref[second, 0, :, cols] = dot_nn(p[2], do_hi).astype(BF16)
        dq_lo = dot_tn(ds[0], k_lo)
        dq_hi = dot_tn(ds[1], k_lo) + dot_tn(ds[2], k_hi)
        dk_lo = dot_nn(ds[0], q_lo) + dot_nn(ds[1], q_hi)
        dk_hi = dot_nn(ds[2], q_hi)
        for pair, src, inv, gain, acc, proj, part_ref in (((dq_lo, dq_hi), q0_ref, iq_ref, gq_ref, acc_q, proj_q, gqp_ref),
                                                          ((dk_lo, dk_hi), k0_ref, ik_ref, gk_ref, acc_k, proj_k, gkp_ref)):
            total = jnp.zeros((8, HEAD_DIM), F32)
            for g, rows, slot in zip(pair, (lo, hi), (first, second)):
                g = (g * cos_ref[rows, :] - pltpu.roll(g, HEAD_DIM // 2, 1) * sin_ref[rows, :]) * inv[slot, 0, :, :]
                vals = src[slot, 0, :, cols].astype(F32)
                total += jnp.sum((g * vals).reshape(tok_len // 8, 8, HEAD_DIM), axis=0)
                g = g * gain[:, cols]
                proj[rows, :] += g * vals
                acc[rows, cols] = g
            part_ref[:, cols] += total

    run_heads(n_heads, (scores, softmax, grads))

    for proj, inv in ((proj_q, iq_ref), (proj_k, ik_ref)):
        for rows, slot in ((lo, first), (hi, second)):
            i = inv[slot, 0, :, :]
            proj[rows, :] = jnp.sum(proj[rows, :], axis=-1, keepdims=True) * (1.0 / width) * i * i

    def finish(r, carry):
        rows = pl.ds(r * ROWS, ROWS)
        for acc, src, proj, dst in ((acc_q, q0_ref, proj_q, dq_ref), (acc_k, k0_ref, proj_k, dk_ref)):
            for slot in range(2):
                pos = pl.ds(pl.multiple_of((side if slot == 0 else 1 - side) * tok_len + r * ROWS, ROWS), ROWS)
                c = proj[pos, :]
                for h in range(n_heads):
                    cols = slice(h * HEAD_DIM, (h + 1) * HEAD_DIM)
                    dst[slot, 0, rows, cols] = (acc[pos, cols] - src[slot, 0, rows, cols].astype(F32) * c).astype(BF16)
        return carry

    lax.fori_loop(0, tok_len // ROWS, finish, 0)


def attn_bwd(side, chunk, q_rot, k_rot, v, d_out, q0, k0, inv_q, inv_k, lse, gain_q, gain_k, cos, sin):
    _, n_seq, tok_len, width = d_out.shape
    seq_len = 2 * tok_len
    first = chunk * n_seq
    halves = pl.BlockSpec((2, 1, tok_len, width), lambda j, s: (0, first + j, 0, 0))
    part_halves = pl.BlockSpec((2, 1, tok_len, width), lambda j, s: (0, j, 0, 0))
    whole = pl.BlockSpec((1, seq_len, width), lambda j, s: (first + j, 0, 0))
    inv = pl.BlockSpec((2, 1, tok_len, HEAD_DIM), lambda j, s: (0, first + j, 0, 0))
    vec = pl.BlockSpec((1, width), lambda j, s: (0, 0))
    part = pl.BlockSpec((8, width), lambda j, s: (0, 0))
    tab = pl.BlockSpec((seq_len, HEAD_DIM), lambda j, s: (0, 0))
    n_heads = width // HEAD_DIM
    square = (3, tok_len, tok_len)
    return pl.pallas_call(
        attn_bwd_kernel,
        grid_spec=pltpu.PrefetchScalarGridSpec(
            num_scalar_prefetch=1, grid=(n_seq,),
            in_specs=[whole, whole, halves, part_halves, halves, halves, inv, inv,
                      pl.BlockSpec((1, n_heads, 8, seq_len), lambda j, s: (first + j, 0, 0, 0)), vec, vec, tab, tab],
            out_specs=[part_halves, part_halves, part_halves, part, part],
            scratch_shapes=[pltpu.VMEM((seq_len, width), F32)] * 2 + [pltpu.VMEM((seq_len, HEAD_DIM), F32)] * 2
            + [[pltpu.VMEM(square, F32)] * 2] * 2 + [[pltpu.VMEM(square, BF16)] * 2] * 2),
        out_shape=[jax.ShapeDtypeStruct(d_out.shape, BF16)] * 3 + [jax.ShapeDtypeStruct((8, width), F32)] * 2,
        compiler_params=pltpu.CompilerParams(vmem_limit_bytes=VMEM_BYTES),
        cost_estimate=pl.CostEstimate(
            flops=n_seq * n_heads * 2 * 10 * tok_len * tok_len * 3 * HEAD_DIM * 2,
            bytes_accessed=n_seq * seq_len * width * 18, transcendentals=n_seq * n_heads * 3 * tok_len * tok_len),
        name="attn_bwd",
    )(side, q_rot, k_rot, v, d_out, q0, k0, inv_q, inv_k, lse, gain_q, gain_k, cos, sin)


def tile_of(n, most):
    return most if n % most == 0 else n


def matmul_kernel(side_ref, a_ref, b_ref, *rest):
    rest[-1][...] = dot_nn(a_ref[...], b_ref[...]).astype(BF16)


def matmul(side, a, b, out_rows, out_block, n_blocks, own=False, into=None):
    depth, width = b.shape
    rows = out_rows // 4
    tile = tile_of(width, 1024)
    row_block = (lambda i, s: s[0] * n_blocks + i) if own else (lambda i, s: i)
    specs = [pl.BlockSpec((rows, depth), lambda i, j, s: (row_block(i, s), 0)), pl.BlockSpec((depth, tile), lambda i, j, s: (0, j))]
    args = [side, a, b]
    if into is not None:
        specs.append(pl.BlockSpec(memory_space=pl.ANY))
        args.append(into)
    return pl.pallas_call(
        matmul_kernel,
        grid_spec=pltpu.PrefetchScalarGridSpec(
            num_scalar_prefetch=1, grid=(n_blocks, width // tile), in_specs=specs,
            out_specs=pl.BlockSpec((rows, tile), lambda i, j, s: (out_block + i, j))),
        out_shape=jax.ShapeDtypeStruct((out_rows, width), BF16),
        input_output_aliases={} if into is None else {3: 0},
        compiler_params=pltpu.CompilerParams(vmem_limit_bytes=VMEM_BYTES),
        cost_estimate=pl.CostEstimate(flops=2 * n_blocks * rows * depth * width, transcendentals=0,
                                      bytes_accessed=2 * (2 * n_blocks * rows * width + depth * width)),
        name="matmul",
    )(*args)


def matmul_nt_kernel(a_ref, b_ref, o_ref):
    o_ref[...] = dot_nt(a_ref[...], b_ref[...]).astype(BF16)


def matmul_nt(a, b):
    n_rows, depth = a.shape
    width = b.shape[0]
    rows, tile = n_rows // 2, tile_of(width, 1024)
    return pl.pallas_call(
        matmul_nt_kernel, grid=(2, width // tile),
        in_specs=[pl.BlockSpec((rows, depth), lambda i, j: (i, 0)), pl.BlockSpec((tile, depth), lambda i, j: (j, 0))],
        out_specs=pl.BlockSpec((rows, tile), lambda i, j: (i, j)),
        out_shape=jax.ShapeDtypeStruct((n_rows, width), BF16),
        compiler_params=pltpu.CompilerParams(vmem_limit_bytes=VMEM_BYTES),
        cost_estimate=pl.CostEstimate(flops=2 * n_rows * depth * width, transcendentals=0,
                                      bytes_accessed=2 * (2 * n_rows * width + depth * width)),
        name="matmul_nt",
    )(a, b)


def wgrad_kernel(side_ref, *refs):
    *lhs, d0_ref, d1_ref, o_ref = refs
    part = d0_ref.shape[0] // 2
    if len(lhs) == 1:
        blocks = [lhs[0][i * part:(i + 1) * part, :] for i in range(4)]
    else:
        blocks = [lhs[0][:part, :], lhs[0][part:, :], lhs[1][...], lhs[2][...]]
    o_ref[...] = (dot_tn(blocks[0], d0_ref[:part, :]) + dot_tn(blocks[1], d1_ref[:part, :])
                  + dot_tn(blocks[2], d0_ref[part:, :]) + dot_tn(blocks[3], d1_ref[part:, :]))


def wgrad(side, lhs, d0, d1, part, n_parts):
    n_rows = d0.shape[0]
    width = d0.shape[1]
    n_cols = width // n_parts
    tall, wide = tile_of(width, 1024), tile_of(n_cols, 512)
    shift = part * n_cols // wide
    if len(lhs) == 1:
        lhs_specs = [pl.BlockSpec((2 * n_rows, tall), lambda i, j, s: (0, i))]
    else:
        lhs_specs = [pl.BlockSpec((n_rows, tall), lambda i, j, s: (s[0], i))]
        lhs_specs += [pl.BlockSpec((n_rows // 2, tall), lambda i, j, s: (0, i))] * 2
    return pl.pallas_call(
        wgrad_kernel,
        grid_spec=pltpu.PrefetchScalarGridSpec(
            num_scalar_prefetch=1, grid=(width // tall, n_cols // wide),
            in_specs=lhs_specs + [pl.BlockSpec((n_rows, wide), lambda i, j, s: (0, shift + j))] * 2,
            out_specs=pl.BlockSpec((tall, wide), lambda i, j, s: (i, j))),
        out_shape=jax.ShapeDtypeStruct((width, n_cols), F32),
        compiler_params=pltpu.CompilerParams(vmem_limit_bytes=VMEM_BYTES),
        cost_estimate=pl.CostEstimate(flops=4 * n_rows * width * n_cols, transcendentals=0, bytes_accessed=12 * n_rows * width),
        name="wgrad",
    )(side, *lhs, d0, d1)


def grad_x_kernel(side_ref, dq_ref, dk_ref, dv_ref, wq_ref, wk_ref, wv_ref, gy_ref, *rest):
    total = dot_nt(dq_ref[...], wq_ref[...]) + dot_nt(dk_ref[...], wk_ref[...]) + dot_nt(dv_ref[...], wv_ref[...])
    rest[-1][...] = (total + gy_ref[...].astype(F32)).astype(BF16)


def grad_x_rows(side, chunk, slot, d, weights, gy, out_rows, into=None):
    width = d[0].shape[1]
    n_rows = d[0].shape[0] // 2
    rows, tile = tile_of(n_rows, 512), tile_of(width, 512)
    steps = n_rows // rows
    row = pl.BlockSpec((rows, width), lambda i, j, s: (slot * steps + i, 0))
    weight = pl.BlockSpec((tile, width), lambda i, j, s: (j, 0))
    place = (lambda i, s: (s[0] * N_CHUNKS + chunk) * steps + i) if slot == 0 else (lambda i, s: i)
    out = pl.BlockSpec((rows, tile), lambda i, j, s: (place(i, s), j))
    specs, args = [row] * 3 + [weight] * 3 + [out], [side, *d, *weights, gy]
    if into is not None:
        specs.append(pl.BlockSpec(memory_space=pl.ANY))
        args.append(into)
    return pl.pallas_call(
        grad_x_kernel,
        grid_spec=pltpu.PrefetchScalarGridSpec(
            num_scalar_prefetch=1, grid=(steps, width // tile), in_specs=specs, out_specs=out),
        out_shape=jax.ShapeDtypeStruct((out_rows, width), BF16),
        input_output_aliases={} if into is None else {8: 0},
        compiler_params=pltpu.CompilerParams(vmem_limit_bytes=VMEM_BYTES),
        cost_estimate=pl.CostEstimate(flops=6 * n_rows * width * width, transcendentals=0,
                                      bytes_accessed=10 * n_rows * width + 6 * width * width),
        name="grad_x",
    )(*args)


def post_kernel(side_ref, a_ref, x_own_ref, x_peer_ref, gy_own_ref, gy_peer_ref, gain_ref, *rest):
    y_own_ref, y_peer_ref, ga_ref, part_ref = rest[-4:]
    step, half = pl.program_id(0), pl.num_programs(0) // 2

    @pl.when(step == 0)
    def _():
        part_ref[...] = jnp.zeros_like(part_ref)

    def run(x_ref, gy_ref, y_ref):
        def rows_step(r, carry):
            rows = pl.ds(r * ROWS, ROWS)
            a = a_ref[rows, :].astype(F32)
            inv = lax.rsqrt(jnp.mean(a * a, axis=-1, keepdims=True) + RMS_EPSILON)
            hat = a * inv
            gain = gain_ref[...]
            y_ref[rows, :] = (x_ref[rows, :].astype(F32) + hat * gain).astype(BF16)
            gy = gy_ref[rows, :].astype(F32)
            prod = gy * hat
            part_ref[...] += prod[:8] + prod[8:]
            proj = jnp.mean(prod * gain, axis=-1, keepdims=True)
            ga_ref[rows, :] = (inv * (gy * gain - hat * proj)).astype(BF16)
            return carry

        lax.fori_loop(0, a_ref.shape[0] // ROWS, rows_step, 0, unroll=4)

    @pl.when(step < half)
    def _():
        run(x_peer_ref, gy_peer_ref, y_peer_ref)

    @pl.when(step >= half)
    def _():
        run(x_own_ref, gy_own_ref, y_own_ref)


def post_norm(side, chunk, a, x, x_peer, gy, gy_peer, gain, into=None):
    n_peer, width = x_peer.shape
    block = min(256, n_peer)
    half = n_peer // block
    all_half = N_CHUNKS * half

    def peer(i, s):
        return jnp.minimum(i, half - 1), 0

    def own(i, s):
        return (s[0] * N_CHUNKS + chunk) * half + jnp.maximum(i - half, 0), 0

    def a_rows(i, s):
        return jnp.where(i < half, all_half + chunk * half + i, chunk * half + i - half), 0

    def ga_rows(i, s):
        return jnp.where(i < half, half + i, i - half), 0

    def spec(index):
        return pl.BlockSpec((block, width), index)

    specs = [spec(a_rows), spec(own), spec(peer), spec(own), spec(peer), pl.BlockSpec((1, width), lambda i, s: (0, 0))]
    args = [side, a, x, x_peer, gy, gy_peer, gain]
    if into is not None:
        specs.append(pl.BlockSpec(memory_space=pl.ANY))
        args.append(into)
    return pl.pallas_call(
        post_kernel,
        grid_spec=pltpu.PrefetchScalarGridSpec(
            num_scalar_prefetch=1, grid=(2 * half,), in_specs=specs,
            out_specs=[spec(own), spec(peer), spec(ga_rows), pl.BlockSpec((8, width), lambda i, s: (0, 0))]),
        out_shape=[jax.ShapeDtypeStruct(x.shape, BF16), jax.ShapeDtypeStruct(x_peer.shape, BF16),
                   jax.ShapeDtypeStruct((2 * n_peer, width), BF16), jax.ShapeDtypeStruct((8, width), F32)],
        input_output_aliases={} if into is None else {7: 0},
        compiler_params=pltpu.CompilerParams(vmem_limit_bytes=VMEM_BYTES),
        cost_estimate=pl.CostEstimate(flops=2 * n_peer * width * 2000, bytes_accessed=n_peer * width * 20, transcendentals=n_peer),
        name="post_norm",
    )(*args)


def solution(mesh):
    tok_spec = P('fsdp', 'sp', None)
    row_spec = P('fsdp', None)
    vec_spec = P('fsdp')
    swap = [(0, 1), (1, 0)]

    def body(x, grad_y, wq_rows, wk_rows, wv_rows, wo_rows, gq_rows, gk_rows, gpost_rows):
        n_batch, tok_len, width = x.shape
        n_own = n_batch // 2
        n_seq = n_own // N_CHUNKS
        n_part = n_seq * tok_len
        all_rows = n_batch * tok_len
        chunks = range(N_CHUNKS)
        my_side = lax.axis_index('sp')
        side = my_side.astype(jnp.int32).reshape(1)
        peer_start = (1 - my_side) * n_own

        def send(part):
            return lax.ppermute(part, 'sp', swap)

        def fetch(array):
            parts = [lax.dynamic_slice_in_dim(array, peer_start + c * n_seq, n_seq) for c in chunks]
            return [send(parts[c]).reshape(n_part, width) for c in chunks]

        x_peer = fetch(x)
        gy_peer = fetch(grad_y)
        x_flat, gy_flat = x.reshape(all_rows, width), grad_y.reshape(all_rows, width)

        w_q, w_k, w_v, w_o = (lax.all_gather(w, 'fsdp', axis=0, tiled=True) for w in (wq_rows, wk_rows, wv_rows, wo_rows))
        gains = lax.all_gather(jnp.stack([gq_rows, gk_rows, gpost_rows]), 'fsdp', axis=1, tiled=True)
        gain_q, gain_k, gain_post = gains[0:1], gains[1:2], gains[2:3]
        cos, sin = rope_tables(2 * tok_len)

        def halves(a):
            return a.reshape(2, a.shape[0] // (2 * tok_len), tok_len, width)

        def flat(a):
            return a.reshape(-1, width)

        def project(w):
            out = matmul(side, x_flat, w, all_rows, 0, 2, own=True)
            for c in chunks:
                out = matmul(side, x_peer[c], w, all_rows, 2 + c, 1, into=out)
            return halves(out)

        q0, k0, v = project(w_q), project(w_k), project(w_v)
        o, q_rot, k_rot, inv_q, inv_k, lse = attn_fwd(side, q0, k0, v, gain_q, gain_k, cos, sin)
        a_lin = matmul(side, flat(o), w_o, all_rows, 0, 4)

        y, ga, y_peer, post_parts, grads = None, [], [], [], []
        for c in chunks:
            y, y_send, ga_c, part = post_norm(side, c, a_lin, x_flat, x_peer[c], gy_flat, gy_peer[c], gain_post, into=y)
            ga.append(ga_c)
            post_parts.append(part)
            y_peer.append(send(y_send.reshape(n_seq, tok_len, width)))
        y = y.reshape(x.shape)
        for c in chunks:
            y = lax.dynamic_update_slice_in_dim(y, y_peer[c], peer_start + c * n_seq, 0)

        for c in chunks:
            d_o = halves(matmul_nt(ga[c], w_o))
            grads.append(attn_bwd(side, c, q_rot, k_rot, v, d_o, q0, k0, inv_q, inv_k, lse, gain_q, gain_k,
                                  cos * HEAD_DIM ** -0.5, sin * HEAD_DIM ** -0.5))

        def weight_grad(lhs, d, n_parts=1):
            out = []
            for i in range(n_parts):
                part = wgrad(side, lhs, *d, i, n_parts)
                rows = lax.psum_scatter(part, 'fsdp', scatter_dimension=0, tiled=True)
                out.append(rows + send(rows))
            return out[0] if n_parts == 1 else jnp.concatenate(out, axis=1)

        d_q, d_k, d_v = ([flat(g[i]) for g in grads] for i in range(3))
        g_wo = weight_grad((flat(o),), ga)
        g_wv = weight_grad((x_flat, *x_peer), d_v)
        g_wk = weight_grad((x_flat, *x_peer), d_k)
        g_wq = weight_grad((x_flat, *x_peer), d_q, 2)

        gx_peer, grad_x = [], None
        for c in chunks:
            gx = grad_x_rows(side, c, 1, (d_q[c], d_k[c], d_v[c]), (w_q, w_k, w_v), gy_peer[c], n_part)
            gx_peer.append(send(gx.reshape(n_seq, tok_len, width)))
        for c in chunks:
            grad_x = grad_x_rows(side, c, 0, (d_q[c], d_k[c], d_v[c]), (w_q, w_k, w_v), gy_flat, all_rows, into=grad_x)
        grad_x = grad_x.reshape(x.shape)
        for c in chunks:
            grad_x = lax.dynamic_update_slice_in_dim(grad_x, gx_peer[c], peer_start + c * n_seq, 0)

        parts = jnp.stack([sum(g[3] for g in grads).sum(0), sum(g[4] for g in grads).sum(0), sum(post_parts).sum(0)])
        for axis, flip in (("sp", 1), ("fsdp", 1), ("fsdp", 2), ("fsdp", 4)):
            parts = parts + lax.ppermute(parts, axis, [(d, d ^ flip) for d in range(mesh.shape[axis])])
        n_vec = gq_rows.shape[0]
        g_vec = lax.dynamic_slice_in_dim(parts, lax.axis_index('fsdp') * n_vec, n_vec, axis=1)
        return y, grad_x, g_wq, g_wk, g_wv, g_wo, g_vec[0], g_vec[1], g_vec[2]

    specs = (tok_spec, tok_spec, row_spec, row_spec, row_spec, row_spec, vec_spec, vec_spec, vec_spec)
    return jax.shard_map(body, mesh=mesh, in_specs=specs, out_specs=specs, check_vma=False)
```

```python
import functools

import jax
import jax.numpy as jnp
from jax import lax
from jax.experimental import pallas as pl
from jax.experimental.pallas import tpu as pltpu
from jax.sharding import PartitionSpec as P


HEAD_DIM = 128
RMS_EPSILON = 1e-6
ROPE_THETA = 500000.0
LOG2E = 1.4426950408889634
N_CHUNKS = 2
F32 = jnp.float32
BF16 = jnp.bfloat16
VMEM_BYTES = 58 * 1024 * 1024
ROWS = 16


def rope_tables(seq_len):
    half_dim = HEAD_DIM // 2
    inv_freq = ROPE_THETA ** (-jnp.arange(half_dim, dtype=F32) * (2.0 / HEAD_DIM))
    angles = jnp.arange(seq_len).astype(F32)[:, None] * inv_freq[None, :]
    cos, sin = jnp.cos(angles), jnp.sin(angles)
    return jnp.concatenate([cos, cos], axis=1), jnp.concatenate([-sin, sin], axis=1)


def dot_nn(a, b):
    return lax.dot_general(a, b, (((1,), (0,)), ((), ())), preferred_element_type=F32)


def dot_nt(a, b):
    return lax.dot_general(a, b, (((1,), (1,)), ((), ())), preferred_element_type=F32)


def dot_tn(a, b):
    return lax.dot_general(a, b, (((0,), (0,)), ((), ())), preferred_element_type=F32)


def head_cols(h):
    return pl.ds(pl.multiple_of(h * HEAD_DIM, HEAD_DIM), HEAD_DIM)


def run_heads(n_heads, stages):
    depth = len(stages)

    def step(h, parity, lo, hi):
        for d in reversed(range(depth)):
            if lo <= d <= hi:
                stages[d](h - d, (parity + d) % 2)

    for h in range(depth - 1):
        step(h, h % 2, 0, h)

    def pair(i, carry):
        h = 2 * i + depth - 1
        step(h, (depth - 1) % 2, 0, depth)
        step(h + 1, depth % 2, 0, depth)
        return carry

    n_full = n_heads - (depth - 1)
    lax.fori_loop(0, n_full // 2, pair, 0)
    for h in range(depth - 1 + n_full // 2 * 2, n_heads):
        step(h, h % 2, 0, depth)
    for h in range(n_heads, n_heads + depth - 1):
        step(h, h % 2, h - n_heads + 1, depth)


def seen_pieces(half, c, part, tok_len):
    diagonal = 2 * half
    pieces = [(1, 0, tok_len)] if half else []
    if c:
        pieces.append((diagonal, 0, c))
    return pieces + [(diagonal, c, c + part)]


def store_scores(out, a_lo, a_hi, b_lo, b_hi, part):
    for block, a, b in ((0, a_lo, b_lo), (2, a_hi, b_hi)):
        for c in range(0, a.shape[0], part):
            out[block, c:c + part, c:] = dot_nt(a[c:c + part], b[c:])
    out[1] = dot_nt(a_lo, b_hi)


def clear_unseen(bufs, part):
    @pl.when(pl.program_id(0) == 0)
    def _():
        for buf in bufs:
            for block in (0, 2):
                for c in range(part, buf.shape[1], part):
                    buf[block, c:c + part, :c] = jnp.zeros((part, c), buf.dtype)


def pick_halves(side, own, peer):
    mine_first = side == 0
    return jnp.where(mine_first, own, peer), jnp.where(mine_first, peer, own)


def attn_fwd_kernel(side_ref, q0_ref, k0_ref, v_ref, gq_ref, gk_ref, cos_ref, sin_ref,
                    o_ref, qr_ref, kr_ref, iq_ref, ik_ref, lse_ref, s_bufs, p_bufs):
    side = side_ref[0]
    tok_len, width = q0_ref.shape[2], q0_ref.shape[3]
    n_heads = width // HEAD_DIM
    scale = LOG2E * HEAD_DIM ** -0.5
    first, second = side, 1 - side

    def stats(r, carry):
        rows = pl.ds(r * ROWS, ROWS)
        for src, dst in ((q0_ref, iq_ref), (k0_ref, ik_ref)):
            for slot in range(2):
                vals = src[slot, 0, rows, :].astype(F32)
                inv = lax.rsqrt(jnp.mean(vals * vals, axis=-1, keepdims=True) + RMS_EPSILON)
                dst[slot, 0, rows, :] = jnp.broadcast_to(inv, (ROWS, HEAD_DIM))
        return carry

    lax.fori_loop(0, tok_len // ROWS, stats, 0, unroll=4 if tok_len >= 4 * ROWS else 1)
    part = min(128, tok_len)
    keep = (lax.broadcasted_iota(jnp.int32, (part, part), 0) <= lax.broadcasted_iota(jnp.int32, (part, part), 1))
    clear_unseen(p_bufs, part)

    def scores(h, parity):
        cols = head_cols(h)
        rot = []
        for src, inv, gain, dst in ((q0_ref, iq_ref, gq_ref, qr_ref), (k0_ref, ik_ref, gk_ref, kr_ref)):
            slots = []
            for slot in range(2):
                pos = pl.ds(pl.multiple_of((side if slot == 0 else 1 - side) * tok_len, tok_len), tok_len)
                u = src[slot, 0, :, cols].astype(F32) * inv[slot, 0, :, :] * gain[:, cols]
                slots.append((u * cos_ref[pos, :] + pltpu.roll(u, HEAD_DIM // 2, 1) * sin_ref[pos, :]).astype(BF16))
            lo, hi = pick_halves(side, *slots)
            dst[0, :tok_len, cols] = lo
            dst[0, tok_len:, cols] = hi
            rot += [lo, hi]
        q_lo, q_hi, k_lo, k_hi = rot
        store_scores(s_bufs[parity], k_lo, k_hi, q_lo, q_hi, part)

    def softmax(h, parity):
        s, p = s_bufs[parity], p_bufs[parity]
        for c in range(0, tok_len, part):
            cols = slice(c, c + part)
            for half in range(2):
                pieces = seen_pieces(half, c, part, tok_len)
                raw = [s[b, i:j, cols] for b, i, j in pieces]
                raw[-1] = jnp.where(keep, raw[-1], -1e30)
                top = functools.reduce(jnp.maximum, [jnp.max(r, axis=0, keepdims=True) for r in raw])
                prob = [jnp.exp2((r - top) * scale) for r in raw]
                total = sum(jnp.sum(r, axis=0, keepdims=True) for r in prob)
                rec = 1.0 / total
                for r, (b, i, j) in zip(prob, pieces):
                    p[b, i:j, cols] = (r * rec).astype(BF16)
                lse = top * scale + jnp.log2(total)
                lse_ref[0, h, :, half * tok_len + c:half * tok_len + c + part] = jnp.broadcast_to(lse, (8, part))

    def mix(h, parity):
        cols = head_cols(h)
        p = p_bufs[parity]
        v_lo, v_hi = v_ref[first, 0, :, cols], v_ref[second, 0, :, cols]
        o_ref[first, 0, :, cols] = dot_tn(p[0], v_lo).astype(BF16)
        o_ref[second, 0, :, cols] = (dot_tn(p[1], v_lo) + dot_tn(p[2], v_hi)).astype(BF16)

    run_heads(n_heads, (scores, softmax, mix))


def attn_fwd(side, q0, k0, v, gain_q, gain_k, cos, sin):
    _, n_seq, tok_len, width = q0.shape
    seq_len = 2 * tok_len
    halves = pl.BlockSpec((2, 1, tok_len, width), lambda j, s: (0, j, 0, 0))
    whole = pl.BlockSpec((1, seq_len, width), lambda j, s: (j, 0, 0))
    inv = pl.BlockSpec((2, 1, tok_len, HEAD_DIM), lambda j, s: (0, j, 0, 0))
    vec = pl.BlockSpec((1, width), lambda j, s: (0, 0))
    tab = pl.BlockSpec((seq_len, HEAD_DIM), lambda j, s: (0, 0))
    n_heads = width // HEAD_DIM
    square = (3, tok_len, tok_len)
    return pl.pallas_call(
        attn_fwd_kernel,
        grid_spec=pltpu.PrefetchScalarGridSpec(
            num_scalar_prefetch=1, grid=(n_seq,),
            in_specs=[halves, halves, halves, vec, vec, tab, tab],
            out_specs=[halves, whole, whole, inv, inv, pl.BlockSpec((1, n_heads, 8, seq_len), lambda j, s: (j, 0, 0, 0))],
            scratch_shapes=[[pltpu.VMEM(square, F32)] * 2, [pltpu.VMEM(square, BF16)] * 2]),
        out_shape=[jax.ShapeDtypeStruct(q0.shape, BF16)]
        + [jax.ShapeDtypeStruct((n_seq, seq_len, width), BF16)] * 2
        + [jax.ShapeDtypeStruct((2, n_seq, tok_len, HEAD_DIM), F32)] * 2 + [jax.ShapeDtypeStruct((n_seq, n_heads, 8, seq_len), F32)],
        compiler_params=pltpu.CompilerParams(vmem_limit_bytes=VMEM_BYTES),
        cost_estimate=pl.CostEstimate(
            flops=n_seq * n_heads * 2 * 4 * tok_len * tok_len * 3 * HEAD_DIM * 2,
            bytes_accessed=n_seq * seq_len * width * 12, transcendentals=n_seq * n_heads * 3 * tok_len * tok_len),
        name="attn_fwd",
    )(side, q0, k0, v, gain_q, gain_k, cos, sin)


def attn_bwd_kernel(side_ref, qr_ref, kr_ref, v_ref, do_ref, q0_ref, k0_ref, iq_ref, ik_ref, lse_ref, gq_ref, gk_ref, cos_ref, sin_ref,
                    dq_ref, dk_ref, dv_ref, gqp_ref, gkp_ref,
                    acc_q, acc_k, proj_q, proj_k, s_bufs, d_bufs, p_bufs, ds_bufs):
    side = side_ref[0]
    tok_len, width = q0_ref.shape[2], q0_ref.shape[3]
    n_heads = width // HEAD_DIM
    scale = LOG2E * HEAD_DIM ** -0.5
    first, second = side, 1 - side
    lo, hi = slice(0, tok_len), slice(tok_len, 2 * tok_len)

    @pl.when(pl.program_id(0) == 0)
    def _():
        gqp_ref[...] = jnp.zeros_like(gqp_ref)
        gkp_ref[...] = jnp.zeros_like(gkp_ref)

    part = min(128, tok_len)
    keep = (lax.broadcasted_iota(jnp.int32, (part, part), 0) <= lax.broadcasted_iota(jnp.int32, (part, part), 1))
    clear_unseen((*p_bufs, *ds_bufs), part)
    proj_q[...] = jnp.zeros_like(proj_q)
    proj_k[...] = jnp.zeros_like(proj_k)

    def scores(h, parity):
        cols = head_cols(h)
        k_lo, k_hi = kr_ref[0, lo, cols], kr_ref[0, hi, cols]
        q_lo, q_hi = qr_ref[0, lo, cols], qr_ref[0, hi, cols]
        v_lo, v_hi = v_ref[first, 0, :, cols], v_ref[second, 0, :, cols]
        do_lo, do_hi = do_ref[first, 0, :, cols], do_ref[second, 0, :, cols]
        store_scores(s_bufs[parity], k_lo, k_hi, q_lo, q_hi, part)
        store_scores(d_bufs[parity], v_lo, v_hi, do_lo, do_hi, part)

    def softmax(h, parity):
        s, d, p, ds = s_bufs[parity], d_bufs[parity], p_bufs[parity], ds_bufs[parity]
        for c in range(0, tok_len, part):
            cols = slice(c, c + part)
            for half in range(2):
                pieces = seen_pieces(half, c, part, tok_len)
                lse = lse_ref[0, h, 0:1, half * tok_len + c:half * tok_len + c + part]
                prob = [jnp.exp2(s[b, i:j, cols] * scale - lse) for b, i, j in pieces]
                prob[-1] = jnp.where(keep, prob[-1], 0.0)
                delta = sum(jnp.sum(r * d[b, i:j, cols], axis=0, keepdims=True) for r, (b, i, j) in zip(prob, pieces))
                for r, (b, i, j) in zip(prob, pieces):
                    p[b, i:j, cols] = r.astype(BF16)
                    ds[b, i:j, cols] = (r * (d[b, i:j, cols] - delta)).astype(BF16)

    def grads(h, parity):
        cols = head_cols(h)
        k_lo, k_hi = kr_ref[0, lo, cols], kr_ref[0, hi, cols]
        q_lo, q_hi = qr_ref[0, lo, cols], qr_ref[0, hi, cols]
        do_lo, do_hi = do_ref[first, 0, :, cols], do_ref[second, 0, :, cols]
        p, ds = p_bufs[parity], ds_bufs[parity]
        dv_ref[first, 0, :, cols] = (dot_nn(p[0], do_lo) + dot_nn(p[1], do_hi)).astype(BF16)
        dv_ref[second, 0, :, cols] = dot_nn(p[2], do_hi).astype(BF16)
        dq_lo = dot_tn(ds[0], k_lo)
        dq_hi = dot_tn(ds[1], k_lo) + dot_tn(ds[2], k_hi)
        dk_lo = dot_nn(ds[0], q_lo) + dot_nn(ds[1], q_hi)
        dk_hi = dot_nn(ds[2], q_hi)
        for pair, src, inv, gain, acc, proj, part_ref in (((dq_lo, dq_hi), q0_ref, iq_ref, gq_ref, acc_q, proj_q, gqp_ref),
                                                          ((dk_lo, dk_hi), k0_ref, ik_ref, gk_ref, acc_k, proj_k, gkp_ref)):
            total = jnp.zeros((8, HEAD_DIM), F32)
            for g, rows, slot in zip(pair, (lo, hi), (first, second)):
                g = (g * cos_ref[rows, :] - pltpu.roll(g, HEAD_DIM // 2, 1) * sin_ref[rows, :]) * inv[slot, 0, :, :]
                vals = src[slot, 0, :, cols].astype(F32)
                total += jnp.sum((g * vals).reshape(tok_len // 8, 8, HEAD_DIM), axis=0)
                g = g * gain[:, cols]
                proj[rows, :] += g * vals
                acc[rows, cols] = g
            part_ref[:, cols] += total

    run_heads(n_heads, (scores, softmax, grads))

    for proj, inv in ((proj_q, iq_ref), (proj_k, ik_ref)):
        for rows, slot in ((lo, first), (hi, second)):
            i = inv[slot, 0, :, :]
            proj[rows, :] = jnp.sum(proj[rows, :], axis=-1, keepdims=True) * (1.0 / width) * i * i

    def finish(r, carry):
        rows = pl.ds(r * ROWS, ROWS)
        for acc, src, proj, dst in ((acc_q, q0_ref, proj_q, dq_ref), (acc_k, k0_ref, proj_k, dk_ref)):
            for slot in range(2):
                pos = pl.ds(pl.multiple_of((side if slot == 0 else 1 - side) * tok_len + r * ROWS, ROWS), ROWS)
                c = proj[pos, :]
                for h in range(n_heads):
                    cols = slice(h * HEAD_DIM, (h + 1) * HEAD_DIM)
                    dst[slot, 0, rows, cols] = (acc[pos, cols] - src[slot, 0, rows, cols].astype(F32) * c).astype(BF16)
        return carry

    lax.fori_loop(0, tok_len // ROWS, finish, 0)


def attn_bwd(side, chunk, q_rot, k_rot, v, d_out, q0, k0, inv_q, inv_k, lse, gain_q, gain_k, cos, sin):
    _, n_seq, tok_len, width = d_out.shape
    seq_len = 2 * tok_len
    first = chunk * n_seq
    halves = pl.BlockSpec((2, 1, tok_len, width), lambda j, s: (0, first + j, 0, 0))
    part_halves = pl.BlockSpec((2, 1, tok_len, width), lambda j, s: (0, j, 0, 0))
    whole = pl.BlockSpec((1, seq_len, width), lambda j, s: (first + j, 0, 0))
    inv = pl.BlockSpec((2, 1, tok_len, HEAD_DIM), lambda j, s: (0, first + j, 0, 0))
    vec = pl.BlockSpec((1, width), lambda j, s: (0, 0))
    part = pl.BlockSpec((8, width), lambda j, s: (0, 0))
    tab = pl.BlockSpec((seq_len, HEAD_DIM), lambda j, s: (0, 0))
    n_heads = width // HEAD_DIM
    square = (3, tok_len, tok_len)
    return pl.pallas_call(
        attn_bwd_kernel,
        grid_spec=pltpu.PrefetchScalarGridSpec(
            num_scalar_prefetch=1, grid=(n_seq,),
            in_specs=[whole, whole, halves, part_halves, halves, halves, inv, inv,
                      pl.BlockSpec((1, n_heads, 8, seq_len), lambda j, s: (first + j, 0, 0, 0)), vec, vec, tab, tab],
            out_specs=[part_halves, part_halves, part_halves, part, part],
            scratch_shapes=[pltpu.VMEM((seq_len, width), F32)] * 2 + [pltpu.VMEM((seq_len, HEAD_DIM), F32)] * 2
            + [[pltpu.VMEM(square, F32)] * 2] * 2 + [[pltpu.VMEM(square, BF16)] * 2] * 2),
        out_shape=[jax.ShapeDtypeStruct(d_out.shape, BF16)] * 3 + [jax.ShapeDtypeStruct((8, width), F32)] * 2,
        compiler_params=pltpu.CompilerParams(vmem_limit_bytes=VMEM_BYTES),
        cost_estimate=pl.CostEstimate(
            flops=n_seq * n_heads * 2 * 10 * tok_len * tok_len * 3 * HEAD_DIM * 2,
            bytes_accessed=n_seq * seq_len * width * 18, transcendentals=n_seq * n_heads * 3 * tok_len * tok_len),
        name="attn_bwd",
    )(side, q_rot, k_rot, v, d_out, q0, k0, inv_q, inv_k, lse, gain_q, gain_k, cos, sin)


def tile_of(n, most):
    return most if n % most == 0 else n


def matmul_kernel(side_ref, a_ref, b_ref, *rest):
    rest[-1][...] = dot_nn(a_ref[...], b_ref[...]).astype(BF16)


def matmul(side, a, b, out_rows, out_block, n_blocks, own=False, into=None):
    depth, width = b.shape
    rows = out_rows // 4
    tile = tile_of(width, 1024)
    row_block = (lambda i, s: s[0] * n_blocks + i) if own else (lambda i, s: i)
    specs = [pl.BlockSpec((rows, depth), lambda i, j, s: (row_block(i, s), 0)), pl.BlockSpec((depth, tile), lambda i, j, s: (0, j))]
    args = [side, a, b]
    if into is not None:
        specs.append(pl.BlockSpec(memory_space=pl.ANY))
        args.append(into)
    return pl.pallas_call(
        matmul_kernel,
        grid_spec=pltpu.PrefetchScalarGridSpec(
            num_scalar_prefetch=1, grid=(n_blocks, width // tile), in_specs=specs,
            out_specs=pl.BlockSpec((rows, tile), lambda i, j, s: (out_block + i, j))),
        out_shape=jax.ShapeDtypeStruct((out_rows, width), BF16),
        input_output_aliases={} if into is None else {3: 0},
        compiler_params=pltpu.CompilerParams(vmem_limit_bytes=VMEM_BYTES),
        cost_estimate=pl.CostEstimate(flops=2 * n_blocks * rows * depth * width, transcendentals=0,
                                      bytes_accessed=2 * (2 * n_blocks * rows * width + depth * width)),
        name="matmul",
    )(*args)


def matmul_nt_kernel(a_ref, b_ref, o_ref):
    o_ref[...] = dot_nt(a_ref[...], b_ref[...]).astype(BF16)


def matmul_nt(a, b):
    n_rows, depth = a.shape
    width = b.shape[0]
    rows, tile = n_rows // 2, tile_of(width, 1024)
    return pl.pallas_call(
        matmul_nt_kernel, grid=(2, width // tile),
        in_specs=[pl.BlockSpec((rows, depth), lambda i, j: (i, 0)), pl.BlockSpec((tile, depth), lambda i, j: (j, 0))],
        out_specs=pl.BlockSpec((rows, tile), lambda i, j: (i, j)),
        out_shape=jax.ShapeDtypeStruct((n_rows, width), BF16),
        compiler_params=pltpu.CompilerParams(vmem_limit_bytes=VMEM_BYTES),
        cost_estimate=pl.CostEstimate(flops=2 * n_rows * depth * width, transcendentals=0,
                                      bytes_accessed=2 * (2 * n_rows * width + depth * width)),
        name="matmul_nt",
    )(a, b)


def wgrad_kernel(side_ref, *refs):
    *lhs, d0_ref, d1_ref, o_ref = refs
    part = d0_ref.shape[0] // 2
    if len(lhs) == 1:
        blocks = [lhs[0][i * part:(i + 1) * part, :] for i in range(4)]
    else:
        blocks = [lhs[0][:part, :], lhs[0][part:, :], lhs[1][...], lhs[2][...]]
    o_ref[...] = (dot_tn(blocks[0], d0_ref[:part, :]) + dot_tn(blocks[1], d1_ref[:part, :])
                  + dot_tn(blocks[2], d0_ref[part:, :]) + dot_tn(blocks[3], d1_ref[part:, :]))


def wgrad(side, lhs, d0, d1, part, n_parts):
    n_rows = d0.shape[0]
    width = d0.shape[1]
    n_cols = width // n_parts
    tall, wide = tile_of(width, 1024), tile_of(n_cols, 512)
    shift = part * n_cols // wide
    if len(lhs) == 1:
        lhs_specs = [pl.BlockSpec((2 * n_rows, tall), lambda i, j, s: (0, i))]
    else:
        lhs_specs = [pl.BlockSpec((n_rows, tall), lambda i, j, s: (s[0], i))]
        lhs_specs += [pl.BlockSpec((n_rows // 2, tall), lambda i, j, s: (0, i))] * 2
    return pl.pallas_call(
        wgrad_kernel,
        grid_spec=pltpu.PrefetchScalarGridSpec(
            num_scalar_prefetch=1, grid=(width // tall, n_cols // wide),
            in_specs=lhs_specs + [pl.BlockSpec((n_rows, wide), lambda i, j, s: (0, shift + j))] * 2,
            out_specs=pl.BlockSpec((tall, wide), lambda i, j, s: (i, j))),
        out_shape=jax.ShapeDtypeStruct((width, n_cols), F32),
        compiler_params=pltpu.CompilerParams(vmem_limit_bytes=VMEM_BYTES),
        cost_estimate=pl.CostEstimate(flops=4 * n_rows * width * n_cols, transcendentals=0, bytes_accessed=12 * n_rows * width),
        name="wgrad",
    )(side, *lhs, d0, d1)


def wgrad_pass_kernel(place_ref, *refs):
    *ins, pass_ref, keep_ref = refs
    step, half = pl.program_id(1), pl.num_programs(1) // 2
    for wanted, out_ref in ((step < half, pass_ref), (step >= half, keep_ref)):
        @pl.when(wanted)
        def _():
            wgrad_kernel(place_ref, *ins, out_ref)


def wgrad_pass(place, lhs, d0, d1, part, n_parts):
    n_rows, width = d0.shape
    n_cols = width // n_parts
    tall = width // 8
    wide = tile_of(n_cols, 1024)
    shift = part * n_cols // wide

    def rows(i, s):
        other_core, q = jnp.where(i < 4, 1, 0), lax.rem(i, 4)
        y = lax.rem(s[3] + jnp.where(q < 2, 1, 0), 2)
        x = lax.rem(s[2] + jnp.where(lax.rem(q, 2) == 0, 1, 0), 2)
        return y * 4 + x * 2 + lax.rem(s[1] + other_core, 2)

    lhs_specs = [pl.BlockSpec((n_rows, tall), lambda j, i, s: (s[0], rows(i, s)))]
    lhs_specs += [pl.BlockSpec((n_rows // 2, tall), lambda j, i, s: (0, rows(i, s)))] * 2
    return pl.pallas_call(
        wgrad_pass_kernel,
        grid_spec=pltpu.PrefetchScalarGridSpec(
            num_scalar_prefetch=1, grid=(n_cols // wide, 8),
            in_specs=lhs_specs + [pl.BlockSpec((n_rows, wide), lambda j, i, s: (0, shift + j))] * 2,
            out_specs=[pl.BlockSpec((tall, wide), lambda j, i, s: (jnp.minimum(i, 3), j)),
                       pl.BlockSpec((tall, wide), lambda j, i, s: (jnp.maximum(i - 4, 0), j))]),
        out_shape=[jax.ShapeDtypeStruct((width // 2, n_cols), F32)] * 2,
        compiler_params=pltpu.CompilerParams(vmem_limit_bytes=VMEM_BYTES),
        cost_estimate=pl.CostEstimate(flops=4 * n_rows * width * n_cols, transcendentals=0, bytes_accessed=12 * n_rows * width),
        name="wgrad_pass",
    )(place, *lhs, d0, d1)


def grad_x_kernel(side_ref, dq_ref, dk_ref, dv_ref, wq_ref, wk_ref, wv_ref, gy_ref, *rest):
    total = dot_nt(dq_ref[...], wq_ref[...]) + dot_nt(dk_ref[...], wk_ref[...]) + dot_nt(dv_ref[...], wv_ref[...])
    rest[-1][...] = (total + gy_ref[...].astype(F32)).astype(BF16)


def grad_x_rows(side, chunk, slot, d, weights, gy, out_rows, into=None):
    width = d[0].shape[1]
    n_rows = d[0].shape[0] // 2
    rows, tile = tile_of(n_rows, 512), tile_of(width, 512)
    steps = n_rows // rows
    row = pl.BlockSpec((rows, width), lambda i, j, s: (slot * steps + i, 0))
    weight = pl.BlockSpec((tile, width), lambda i, j, s: (j, 0))
    place = (lambda i, s: (s[0] * N_CHUNKS + chunk) * steps + i) if slot == 0 else (lambda i, s: i)
    out = pl.BlockSpec((rows, tile), lambda i, j, s: (place(i, s), j))
    specs, args = [row] * 3 + [weight] * 3 + [out], [side, *d, *weights, gy]
    if into is not None:
        specs.append(pl.BlockSpec(memory_space=pl.ANY))
        args.append(into)
    return pl.pallas_call(
        grad_x_kernel,
        grid_spec=pltpu.PrefetchScalarGridSpec(
            num_scalar_prefetch=1, grid=(steps, width // tile), in_specs=specs, out_specs=out),
        out_shape=jax.ShapeDtypeStruct((out_rows, width), BF16),
        input_output_aliases={} if into is None else {8: 0},
        compiler_params=pltpu.CompilerParams(vmem_limit_bytes=VMEM_BYTES),
        cost_estimate=pl.CostEstimate(flops=6 * n_rows * width * width, transcendentals=0,
                                      bytes_accessed=10 * n_rows * width + 6 * width * width),
        name="grad_x",
    )(*args)


def post_kernel(side_ref, o_ref, w_ref, x_own_ref, x_peer_ref, gy_own_ref, gy_peer_ref, gain_ref, *rest):
    y_own_ref, y_peer_ref, ga_ref, part_ref, acc_even, acc_odd = rest[-6:]
    step, last = pl.program_id(0), pl.num_programs(0) - 1
    n_rows, width = o_ref.shape
    is_peer = step - 1 < last // 2
    chunk = tile_of(width, 512)
    chunks = [slice(c, c + chunk) for c in range(0, width, chunk)]

    def norm_rows(acc, rows):
        def a_of(cols):
            return acc[rows, cols].astype(BF16).astype(F32)

        def gy_of(cols):
            return jnp.where(is_peer, gy_peer_ref[rows, cols], gy_own_ref[rows, cols]).astype(F32)

        square = cross = jnp.zeros((ROWS, HEAD_DIM), F32)
        for cols in chunks:
            a = a_of(cols)
            mixed = gy_of(cols) * gain_ref[:, cols] * a
            a = a * a
            for h in range(0, chunk, HEAD_DIM):
                square += a[:, h:h + HEAD_DIM]
                cross += mixed[:, h:h + HEAD_DIM]
        inv = lax.rsqrt(jnp.sum(square, axis=-1, keepdims=True) * (1.0 / width) + RMS_EPSILON)
        proj = jnp.sum(cross, axis=-1, keepdims=True) * (1.0 / width) * inv
        for cols in chunks:
            gain = gain_ref[:, cols]
            hat = a_of(cols) * inv
            x = jnp.where(is_peer, x_peer_ref[rows, cols], x_own_ref[rows, cols]).astype(F32)
            y = (x + hat * gain).astype(BF16)
            y_own_ref[rows, cols] = y
            y_peer_ref[rows, cols] = jnp.where(is_peer, y, y_peer_ref[rows, cols])
            gy = gy_of(cols)
            prod = gy * hat
            part_ref[:, cols] += prod[:8] + prod[8:]
            ga_ref[rows, cols] = (inv * (gy * gain - hat * proj)).astype(BF16)

    def project(acc):
        acc[...] = dot_nn(o_ref[...], w_ref[...])

    @pl.when(step == 0)
    def _():
        part_ref[...] = jnp.zeros_like(part_ref)
        project(acc_even)

    for parity, (now, before) in enumerate(((acc_even, acc_odd), (acc_odd, acc_even))):
        @pl.when(jnp.logical_and(lax.rem(step, 2) == parity, jnp.logical_and(step > 0, step < last)))
        def _():
            for r in range(0, n_rows, ROWS):
                norm_rows(before, slice(r, r + ROWS))
            project(now)

    @pl.when(step == last)
    def _():
        def rows_step(r, carry):
            norm_rows(acc_odd, pl.ds(pl.multiple_of(r * ROWS, ROWS), ROWS))
            return carry

        lax.fori_loop(0, n_rows // ROWS, rows_step, 0)


def post_norm(side, chunk, o, w_o, x, x_peer, gy, gy_peer, gain, into=None):
    n_peer, width = x_peer.shape
    block = min(256, n_peer)
    half = n_peer // block
    all_half = N_CHUNKS * half

    def o_rows(i, s):
        i = jnp.minimum(i, 2 * half - 1)
        return jnp.where(i < half, all_half + chunk * half + i, chunk * half + i - half), 0

    def behind(i):
        return jnp.maximum(i - 1, 0)

    def peer(i, s):
        return jnp.minimum(behind(i), half - 1), 0

    def own(i, s):
        return (s[0] * N_CHUNKS + chunk) * half + jnp.maximum(behind(i) - half, 0), 0

    def ga_rows(i, s):
        i = behind(i)
        return jnp.where(i < half, half + i, i - half), 0

    def spec(index):
        return pl.BlockSpec((block, width), index)

    specs = [spec(o_rows), pl.BlockSpec((width, width), lambda i, s: (0, 0), pipeline_mode=pl.Buffered(1)),
             spec(own), spec(peer), spec(own), spec(peer), pl.BlockSpec((1, width), lambda i, s: (0, 0))]
    args = [side, o, w_o, x, x_peer, gy, gy_peer, gain]
    if into is not None:
        specs.append(pl.BlockSpec(memory_space=pl.ANY))
        args.append(into)
    return pl.pallas_call(
        post_kernel,
        grid_spec=pltpu.PrefetchScalarGridSpec(
            num_scalar_prefetch=1, grid=(2 * half + 1,), in_specs=specs,
            out_specs=[spec(own), spec(peer), spec(ga_rows), pl.BlockSpec((8, width), lambda i, s: (0, 0))],
            scratch_shapes=[pltpu.VMEM((block, width), F32)] * 2),
        out_shape=[jax.ShapeDtypeStruct(x.shape, BF16), jax.ShapeDtypeStruct(x_peer.shape, BF16),
                   jax.ShapeDtypeStruct((2 * n_peer, width), BF16), jax.ShapeDtypeStruct((8, width), F32)],
        input_output_aliases={} if into is None else {8: 0},
        compiler_params=pltpu.CompilerParams(vmem_limit_bytes=VMEM_BYTES),
        cost_estimate=pl.CostEstimate(flops=4 * n_peer * width * width, bytes_accessed=n_peer * width * 20, transcendentals=n_peer),
        name="post_norm",
    )(*args)


def solution(mesh):
    tok_spec = P('fsdp', 'sp', None)
    row_spec = P('fsdp', None)
    vec_spec = P('fsdp')
    swap = [(0, 1), (1, 0)]

    def body(x, grad_y, wq_rows, wk_rows, wv_rows, wo_rows, gq_rows, gk_rows, gpost_rows):
        n_batch, tok_len, width = x.shape
        n_own = n_batch // 2
        n_seq = n_own // N_CHUNKS
        n_part = n_seq * tok_len
        all_rows = n_batch * tok_len
        chunks = range(N_CHUNKS)
        my_side = lax.axis_index('sp')
        side = my_side.astype(jnp.int32).reshape(1)
        peer_start = (1 - my_side) * n_own

        def send(part):
            return lax.ppermute(part, 'sp', swap)

        def fetch(array):
            parts = [lax.dynamic_slice_in_dim(array, peer_start + c * n_seq, n_seq) for c in chunks]
            return [send(parts[c]).reshape(n_part, width) for c in chunks]

        x_peer = fetch(x)
        gy_peer = fetch(grad_y)
        x_flat, gy_flat = x.reshape(all_rows, width), grad_y.reshape(all_rows, width)

        w_q, w_k, w_v, w_o = (lax.all_gather(w, 'fsdp', axis=0, tiled=True) for w in (wq_rows, wk_rows, wv_rows, wo_rows))
        gains = lax.all_gather(jnp.stack([gq_rows, gk_rows, gpost_rows]), 'fsdp', axis=1, tiled=True)
        gain_q, gain_k, gain_post = gains[0:1], gains[1:2], gains[2:3]
        cos, sin = rope_tables(2 * tok_len)

        def halves(a):
            return a.reshape(2, a.shape[0] // (2 * tok_len), tok_len, width)

        def flat(a):
            return a.reshape(-1, width)

        def project(w):
            out = matmul(side, x_flat, w, all_rows, 0, 2, own=True)
            for c in chunks:
                out = matmul(side, x_peer[c], w, all_rows, 2 + c, 1, into=out)
            return halves(out)

        q0, k0, v = project(w_q), project(w_k), project(w_v)
        o, q_rot, k_rot, inv_q, inv_k, lse = attn_fwd(side, q0, k0, v, gain_q, gain_k, cos, sin)
        y, ga, y_peer, post_parts, grads = None, [], [], [], []
        for c in chunks:
            y, y_send, ga_c, part = post_norm(side, c, flat(o), w_o, x_flat, x_peer[c], gy_flat, gy_peer[c], gain_post, into=y)
            ga.append(ga_c)
            post_parts.append(part)
            y_peer.append(send(y_send.reshape(n_seq, tok_len, width)))
        y = y.reshape(x.shape)
        for c in chunks:
            y = lax.dynamic_update_slice_in_dim(y, y_peer[c], peer_start + c * n_seq, 0)

        for c in chunks:
            d_o = halves(matmul_nt(ga[c], w_o))
            grads.append(attn_bwd(side, c, q_rot, k_rot, v, d_o, q0, k0, inv_q, inv_k, lse, gain_q, gain_k,
                                  cos * HEAD_DIM ** -0.5, sin * HEAD_DIM ** -0.5))

        def weight_grad(lhs, d, n_parts=1):
            out = []
            for i in range(n_parts):
                part = wgrad(side, lhs, *d, i, n_parts)
                rows = lax.psum_scatter(part, 'fsdp', scatter_dimension=0, tiled=True)
                out.append(rows + send(rows))
            return out[0] if n_parts == 1 else jnp.concatenate(out, axis=1)

        d_q, d_k, d_v = ([flat(g[i]) for g in grads] for i in range(3))
        g_wo = weight_grad((flat(o),), ga)
        g_wv = weight_grad((x_flat, *x_peer), d_v)
        g_wk = weight_grad((x_flat, *x_peer), d_k)

        def exchange(part, flip):
            return lax.ppermute(part, 'fsdp', [(d, d ^ flip) for d in range(8)])

        my_dev = lax.axis_index('fsdp').astype(jnp.int32)
        place = jnp.stack([side[0], my_dev % 2, my_dev // 2 % 2, my_dev // 4])
        quarter = width // 8
        parts_wq = []
        for i in range(2):
            away, keep = wgrad_pass(place, (x_flat, *x_peer), *d_q, i, 2)
            parts_wq.append((keep, exchange(away, 1)))
        for i in range(2):
            keep, near = parts_wq[i]
            far = exchange(keep[:2 * quarter] + near[:2 * quarter], 4)
            parts_wq[i] = keep, near, far
        for i in range(2):
            keep, near, far = parts_wq[i]
            last = exchange(keep[2 * quarter:3 * quarter] + near[2 * quarter:3 * quarter] + far[:quarter], 2)
            total = keep[3 * quarter:] + near[3 * quarter:] + far[quarter:] + last
            parts_wq[i] = total
        g_wq = jnp.concatenate([rows + send(rows) for rows in parts_wq], axis=1)

        gx_peer, grad_x = [], None
        for c in chunks:
            gx = grad_x_rows(side, c, 1, (d_q[c], d_k[c], d_v[c]), (w_q, w_k, w_v), gy_peer[c], n_part)
            gx_peer.append(send(gx.reshape(n_seq, tok_len, width)))
        for c in chunks:
            grad_x = grad_x_rows(side, c, 0, (d_q[c], d_k[c], d_v[c]), (w_q, w_k, w_v), gy_flat, all_rows, into=grad_x)
        grad_x = grad_x.reshape(x.shape)
        for c in chunks:
            grad_x = lax.dynamic_update_slice_in_dim(grad_x, gx_peer[c], peer_start + c * n_seq, 0)

        parts = jnp.stack([sum(g[3] for g in grads).sum(0), sum(g[4] for g in grads).sum(0), sum(post_parts).sum(0)])
        for axis, flip in (("sp", 1), ("fsdp", 1), ("fsdp", 2), ("fsdp", 4)):
            parts = parts + lax.ppermute(parts, axis, [(d, d ^ flip) for d in range(mesh.shape[axis])])
        n_vec = gq_rows.shape[0]
        g_vec = lax.dynamic_slice_in_dim(parts, lax.axis_index('fsdp') * n_vec, n_vec, axis=1)
        return y, grad_x, g_wq, g_wk, g_wv, g_wo, g_vec[0], g_vec[1], g_vec[2]

    specs = (tok_spec, tok_spec, row_spec, row_spec, row_spec, row_spec, vec_spec, vec_spec, vec_spec)
    return jax.shard_map(body, mesh=mesh, in_specs=specs, out_specs=specs, check_vma=False)
```

```python
import functools

import jax
import jax.numpy as jnp
from jax import lax
from jax.experimental import pallas as pl
from jax.experimental.pallas import tpu as pltpu
from jax.sharding import PartitionSpec as P


HEAD_DIM = 128
RMS_EPSILON = 1e-6
ROPE_THETA = 500000.0
LOG2E = 1.4426950408889634
N_CHUNKS = 2
F32 = jnp.float32
BF16 = jnp.bfloat16
VMEM_BYTES = 58 * 1024 * 1024
ROWS = 16

COMPILER_PARAMS = pltpu.CompilerParams(vmem_limit_bytes=VMEM_BYTES)


def cost(flops):
    return pl.CostEstimate(flops=flops, transcendentals=0, bytes_accessed=flops // 500)


def rope_tables(seq_len):
    half_dim = HEAD_DIM // 2
    inv_freq = ROPE_THETA ** (-jnp.arange(half_dim, dtype=F32) * (2.0 / HEAD_DIM))
    angles = jnp.arange(seq_len).astype(F32)[:, None] * inv_freq[None, :]
    cos, sin = jnp.cos(angles), jnp.sin(angles)
    return jnp.concatenate([cos, cos], axis=1), jnp.concatenate([-sin, sin], axis=1)


def dot_nn(a, b):
    return lax.dot_general(a, b, (((1,), (0,)), ((), ())), preferred_element_type=F32)


def dot_nt(a, b):
    return lax.dot_general(a, b, (((1,), (1,)), ((), ())), preferred_element_type=F32)


def dot_tn(a, b):
    return lax.dot_general(a, b, (((0,), (0,)), ((), ())), preferred_element_type=F32)


def head_cols(h):
    return pl.ds(pl.multiple_of(h * HEAD_DIM, HEAD_DIM), HEAD_DIM)


def run_heads(n_heads, stages):
    depth = len(stages)

    def step(h, parity, lo, hi):
        for d in reversed(range(depth)):
            if lo <= d <= hi:
                stages[d](h - d, (parity + d) % 2)

    for h in range(depth - 1):
        step(h, h % 2, 0, h)

    def pair(i, carry):
        h = 2 * i + depth - 1
        step(h, (depth - 1) % 2, 0, depth)
        step(h + 1, depth % 2, 0, depth)
        return carry

    n_full = n_heads - (depth - 1)
    lax.fori_loop(0, n_full // 2, pair, 0)
    for h in range(depth - 1 + n_full // 2 * 2, n_heads):
        step(h, h % 2, 0, depth)
    for h in range(n_heads, n_heads + depth - 1):
        step(h, h % 2, h - n_heads + 1, depth)


def seen_pieces(half, c, part, tok_len):
    diagonal = 2 * half
    pieces = [(1, 0, tok_len)] if half else []
    if c:
        pieces.append((diagonal, 0, c))
    return pieces + [(diagonal, c, c + part)]


def store_scores(out, a_lo, a_hi, b_lo, b_hi, part):
    for block, a, b in ((0, a_lo, b_lo), (2, a_hi, b_hi)):
        for c in range(0, a.shape[0], part):
            out[block, c:c + part, c:] = dot_nt(a[c:c + part], b[c:])
    out[1] = dot_nt(a_lo, b_hi)


def clear_unseen(bufs, part):
    @pl.when(pl.program_id(0) == 0)
    def _():
        for buf in bufs:
            for block in (0, 2):
                for c in range(part, buf.shape[1], part):
                    buf[block, c:c + part, :c] = jnp.zeros((part, c), buf.dtype)


def pick_halves(side, own, peer):
    mine_first = side == 0
    return jnp.where(mine_first, own, peer), jnp.where(mine_first, peer, own)


def attn_fwd_kernel(side_ref, q0_ref, k0_ref, v_ref, gq_ref, gk_ref, cos_ref, sin_ref,
                    o_ref, qr_ref, kr_ref, iq_ref, ik_ref, lse_ref, s_bufs, p_bufs):
    side = side_ref[0]
    tok_len, width = q0_ref.shape[2], q0_ref.shape[3]
    n_heads = width // HEAD_DIM
    scale = LOG2E * HEAD_DIM ** -0.5
    first, second = side, 1 - side

    def stats(r, carry):
        rows = pl.ds(r * ROWS, ROWS)
        for src, dst in ((q0_ref, iq_ref), (k0_ref, ik_ref)):
            for slot in range(2):
                vals = src[slot, 0, rows, :].astype(F32)
                inv = lax.rsqrt(jnp.mean(vals * vals, axis=-1, keepdims=True) + RMS_EPSILON)
                dst[slot, 0, rows, :] = jnp.broadcast_to(inv, (ROWS, HEAD_DIM))
        return carry

    lax.fori_loop(0, tok_len // ROWS, stats, 0, unroll=4 if tok_len >= 4 * ROWS else 1)
    part = min(128, tok_len)
    keep = (lax.broadcasted_iota(jnp.int32, (part, part), 0) <= lax.broadcasted_iota(jnp.int32, (part, part), 1))
    clear_unseen(p_bufs, part)

    def scores(h, parity):
        cols = head_cols(h)
        rot = []
        for src, inv, gain, dst in ((q0_ref, iq_ref, gq_ref, qr_ref), (k0_ref, ik_ref, gk_ref, kr_ref)):
            slots = []
            for slot in range(2):
                pos = pl.ds(pl.multiple_of((side if slot == 0 else 1 - side) * tok_len, tok_len), tok_len)
                u = src[slot, 0, :, cols].astype(F32) * inv[slot, 0, :, :] * gain[:, cols]
                slots.append((u * cos_ref[pos, :] + pltpu.roll(u, HEAD_DIM // 2, 1) * sin_ref[pos, :]).astype(BF16))
            lo, hi = pick_halves(side, *slots)
            dst[0, :tok_len, cols] = lo
            dst[0, tok_len:, cols] = hi
            rot += [lo, hi]
        q_lo, q_hi, k_lo, k_hi = rot
        store_scores(s_bufs[parity], k_lo, k_hi, q_lo, q_hi, part)

    def softmax(h, parity):
        s, p = s_bufs[parity], p_bufs[parity]
        for c in range(0, tok_len, part):
            cols = slice(c, c + part)
            for half in range(2):
                pieces = seen_pieces(half, c, part, tok_len)
                raw = [s[b, i:j, cols] for b, i, j in pieces]
                raw[-1] = jnp.where(keep, raw[-1], -1e30)
                top = functools.reduce(jnp.maximum, [jnp.max(r, axis=0, keepdims=True) for r in raw])
                prob = [jnp.exp2((r - top) * scale) for r in raw]
                total = sum(jnp.sum(r, axis=0, keepdims=True) for r in prob)
                rec = 1.0 / total
                for r, (b, i, j) in zip(prob, pieces):
                    p[b, i:j, cols] = (r * rec).astype(BF16)
                lse = top * scale + jnp.log2(total)
                lse_ref[0, h, :, half * tok_len + c:half * tok_len + c + part] = jnp.broadcast_to(lse, (8, part))

    def mix(h, parity):
        cols = head_cols(h)
        p = p_bufs[parity]
        v_lo, v_hi = v_ref[first, 0, :, cols], v_ref[second, 0, :, cols]
        o_ref[first, 0, :, cols] = dot_tn(p[0], v_lo).astype(BF16)
        o_ref[second, 0, :, cols] = (dot_tn(p[1], v_lo) + dot_tn(p[2], v_hi)).astype(BF16)

    run_heads(n_heads, (scores, softmax, mix))


def attn_fwd(side, q0, k0, v, gain_q, gain_k, cos, sin):
    _, n_seq, tok_len, width = q0.shape
    seq_len = 2 * tok_len
    halves = pl.BlockSpec((2, 1, tok_len, width), lambda j, s: (0, j, 0, 0))
    whole = pl.BlockSpec((1, seq_len, width), lambda j, s: (j, 0, 0))
    inv = pl.BlockSpec((2, 1, tok_len, HEAD_DIM), lambda j, s: (0, j, 0, 0))
    vec = pl.BlockSpec((1, width), lambda j, s: (0, 0))
    tab = pl.BlockSpec((seq_len, HEAD_DIM), lambda j, s: (0, 0))
    n_heads = width // HEAD_DIM
    square = (3, tok_len, tok_len)
    return pl.pallas_call(
        attn_fwd_kernel,
        grid_spec=pltpu.PrefetchScalarGridSpec(
            num_scalar_prefetch=1, grid=(n_seq,),
            in_specs=[halves, halves, halves, vec, vec, tab, tab],
            out_specs=[halves, whole, whole, inv, inv, pl.BlockSpec((1, n_heads, 8, seq_len), lambda j, s: (j, 0, 0, 0))],
            scratch_shapes=[[pltpu.VMEM(square, F32)] * 2, [pltpu.VMEM(square, BF16)] * 2]),
        out_shape=[jax.ShapeDtypeStruct(q0.shape, BF16)]
        + [jax.ShapeDtypeStruct((n_seq, seq_len, width), BF16)] * 2
        + [jax.ShapeDtypeStruct((2, n_seq, tok_len, HEAD_DIM), F32)] * 2 + [jax.ShapeDtypeStruct((n_seq, n_heads, 8, seq_len), F32)],
        compiler_params=COMPILER_PARAMS,
        cost_estimate=cost(12 * n_seq * seq_len * seq_len * width),
        name="attn_fwd",
    )(side, q0, k0, v, gain_q, gain_k, cos, sin)


def attn_bwd_kernel(side_ref, qr_ref, kr_ref, v_ref, do_ref, q0_ref, k0_ref, iq_ref, ik_ref, lse_ref, gq_ref, gk_ref, cos_ref, sin_ref,
                    dq_ref, dk_ref, dv_ref, gqp_ref, gkp_ref,
                    acc_q, acc_k, proj_q, proj_k, s_bufs, d_bufs, p_bufs, ds_bufs):
    side = side_ref[0]
    tok_len, width = q0_ref.shape[2], q0_ref.shape[3]
    n_heads = width // HEAD_DIM
    scale = LOG2E * HEAD_DIM ** -0.5
    first, second = side, 1 - side
    lo, hi = slice(0, tok_len), slice(tok_len, 2 * tok_len)

    @pl.when(pl.program_id(0) == 0)
    def _():
        gqp_ref[...] = jnp.zeros_like(gqp_ref)
        gkp_ref[...] = jnp.zeros_like(gkp_ref)

    part = min(128, tok_len)
    keep = (lax.broadcasted_iota(jnp.int32, (part, part), 0) <= lax.broadcasted_iota(jnp.int32, (part, part), 1))
    clear_unseen((*p_bufs, *ds_bufs), part)
    proj_q[...] = jnp.zeros_like(proj_q)
    proj_k[...] = jnp.zeros_like(proj_k)

    def scores(h, parity):
        cols = head_cols(h)
        k_lo, k_hi = kr_ref[0, lo, cols], kr_ref[0, hi, cols]
        q_lo, q_hi = qr_ref[0, lo, cols], qr_ref[0, hi, cols]
        v_lo, v_hi = v_ref[first, 0, :, cols], v_ref[second, 0, :, cols]
        do_lo, do_hi = do_ref[first, 0, :, cols], do_ref[second, 0, :, cols]
        store_scores(s_bufs[parity], k_lo, k_hi, q_lo, q_hi, part)
        store_scores(d_bufs[parity], v_lo, v_hi, do_lo, do_hi, part)

    def softmax(h, parity):
        s, d, p, ds = s_bufs[parity], d_bufs[parity], p_bufs[parity], ds_bufs[parity]
        for c in range(0, tok_len, part):
            cols = slice(c, c + part)
            for half in range(2):
                pieces = seen_pieces(half, c, part, tok_len)
                lse = lse_ref[0, h, 0:1, half * tok_len + c:half * tok_len + c + part]
                prob = [jnp.exp2(s[b, i:j, cols] * scale - lse) for b, i, j in pieces]
                prob[-1] = jnp.where(keep, prob[-1], 0.0)
                delta = sum(jnp.sum(r * d[b, i:j, cols], axis=0, keepdims=True) for r, (b, i, j) in zip(prob, pieces))
                for r, (b, i, j) in zip(prob, pieces):
                    p[b, i:j, cols] = r.astype(BF16)
                    ds[b, i:j, cols] = (r * (d[b, i:j, cols] - delta)).astype(BF16)

    def grads(h, parity):
        cols = head_cols(h)
        k_lo, k_hi = kr_ref[0, lo, cols], kr_ref[0, hi, cols]
        q_lo, q_hi = qr_ref[0, lo, cols], qr_ref[0, hi, cols]
        do_lo, do_hi = do_ref[first, 0, :, cols], do_ref[second, 0, :, cols]
        p, ds = p_bufs[parity], ds_bufs[parity]
        dv_ref[first, 0, :, cols] = (dot_nn(p[0], do_lo) + dot_nn(p[1], do_hi)).astype(BF16)
        dv_ref[second, 0, :, cols] = dot_nn(p[2], do_hi).astype(BF16)
        dq_lo = dot_tn(ds[0], k_lo)
        dq_hi = dot_tn(ds[1], k_lo) + dot_tn(ds[2], k_hi)
        dk_lo = dot_nn(ds[0], q_lo) + dot_nn(ds[1], q_hi)
        dk_hi = dot_nn(ds[2], q_hi)
        for pair, src, inv, gain, acc, proj, part_ref in (((dq_lo, dq_hi), q0_ref, iq_ref, gq_ref, acc_q, proj_q, gqp_ref),
                                                          ((dk_lo, dk_hi), k0_ref, ik_ref, gk_ref, acc_k, proj_k, gkp_ref)):
            total = jnp.zeros((8, HEAD_DIM), F32)
            for g, rows, slot in zip(pair, (lo, hi), (first, second)):
                g = (g * cos_ref[rows, :] - pltpu.roll(g, HEAD_DIM // 2, 1) * sin_ref[rows, :]) * inv[slot, 0, :, :]
                vals = src[slot, 0, :, cols].astype(F32)
                total += jnp.sum((g * vals).reshape(tok_len // 8, 8, HEAD_DIM), axis=0)
                g = g * gain[:, cols]
                proj[rows, :] += g * vals
                acc[rows, cols] = g
            part_ref[:, cols] += total

    run_heads(n_heads, (scores, softmax, grads))

    for proj, inv in ((proj_q, iq_ref), (proj_k, ik_ref)):
        for rows, slot in ((lo, first), (hi, second)):
            i = inv[slot, 0, :, :]
            proj[rows, :] = jnp.sum(proj[rows, :], axis=-1, keepdims=True) * (1.0 / width) * i * i

    def finish(r, carry):
        rows = pl.ds(r * ROWS, ROWS)
        for acc, src, proj, dst in ((acc_q, q0_ref, proj_q, dq_ref), (acc_k, k0_ref, proj_k, dk_ref)):
            for slot in range(2):
                pos = pl.ds(pl.multiple_of((side if slot == 0 else 1 - side) * tok_len + r * ROWS, ROWS), ROWS)
                c = proj[pos, :]
                for h in range(n_heads):
                    cols = slice(h * HEAD_DIM, (h + 1) * HEAD_DIM)
                    dst[slot, 0, rows, cols] = (acc[pos, cols] - src[slot, 0, rows, cols].astype(F32) * c).astype(BF16)
        return carry

    lax.fori_loop(0, tok_len // ROWS, finish, 0)


def attn_bwd(side, chunk, q_rot, k_rot, v, d_out, q0, k0, inv_q, inv_k, lse, gain_q, gain_k, cos, sin):
    _, n_seq, tok_len, width = d_out.shape
    seq_len = 2 * tok_len
    first = chunk * n_seq
    halves = pl.BlockSpec((2, 1, tok_len, width), lambda j, s: (0, first + j, 0, 0))
    part_halves = pl.BlockSpec((2, 1, tok_len, width), lambda j, s: (0, j, 0, 0))
    whole = pl.BlockSpec((1, seq_len, width), lambda j, s: (first + j, 0, 0))
    inv = pl.BlockSpec((2, 1, tok_len, HEAD_DIM), lambda j, s: (0, first + j, 0, 0))
    vec = pl.BlockSpec((1, width), lambda j, s: (0, 0))
    part = pl.BlockSpec((8, width), lambda j, s: (0, 0))
    tab = pl.BlockSpec((seq_len, HEAD_DIM), lambda j, s: (0, 0))
    n_heads = width // HEAD_DIM
    square = (3, tok_len, tok_len)
    return pl.pallas_call(
        attn_bwd_kernel,
        grid_spec=pltpu.PrefetchScalarGridSpec(
            num_scalar_prefetch=1, grid=(n_seq,),
            in_specs=[whole, whole, halves, part_halves, halves, halves, inv, inv,
                      pl.BlockSpec((1, n_heads, 8, seq_len), lambda j, s: (first + j, 0, 0, 0)), vec, vec, tab, tab],
            out_specs=[part_halves, part_halves, part_halves, part, part],
            scratch_shapes=[pltpu.VMEM((seq_len, width), F32)] * 2 + [pltpu.VMEM((seq_len, HEAD_DIM), F32)] * 2
            + [[pltpu.VMEM(square, F32)] * 2] * 2 + [[pltpu.VMEM(square, BF16)] * 2] * 2),
        out_shape=[jax.ShapeDtypeStruct(d_out.shape, BF16)] * 3 + [jax.ShapeDtypeStruct((8, width), F32)] * 2,
        compiler_params=COMPILER_PARAMS,
        cost_estimate=cost(30 * n_seq * seq_len * seq_len * width),
        name="attn_bwd",
    )(side, q_rot, k_rot, v, d_out, q0, k0, inv_q, inv_k, lse, gain_q, gain_k, cos, sin)


def tile_of(n, most):
    return most if n % most == 0 else n


def matmul_kernel(side_ref, a_ref, b_ref, *rest):
    rest[-1][...] = dot_nn(a_ref[...], b_ref[...]).astype(BF16)


def matmul(side, a, b, out_rows, out_block, n_blocks, own=False, into=None):
    depth, width = b.shape
    rows = out_rows // 4
    tile = tile_of(width, 1024)
    row_block = (lambda i, s: s[0] * n_blocks + i) if own else (lambda i, s: i)
    specs = [pl.BlockSpec((rows, depth), lambda i, j, s: (row_block(i, s), 0)), pl.BlockSpec((depth, tile), lambda i, j, s: (0, j))]
    args = [side, a, b]
    if into is not None:
        specs.append(pl.BlockSpec(memory_space=pl.ANY))
        args.append(into)
    return pl.pallas_call(
        matmul_kernel,
        grid_spec=pltpu.PrefetchScalarGridSpec(
            num_scalar_prefetch=1, grid=(n_blocks, width // tile), in_specs=specs,
            out_specs=pl.BlockSpec((rows, tile), lambda i, j, s: (out_block + i, j))),
        out_shape=jax.ShapeDtypeStruct((out_rows, width), BF16),
        input_output_aliases={} if into is None else {3: 0},
        compiler_params=COMPILER_PARAMS,
        cost_estimate=cost(2 * n_blocks * rows * depth * width),
        name="matmul",
    )(*args)


def matmul_nt_kernel(a_ref, b_ref, o_ref):
    o_ref[...] = dot_nt(a_ref[...], b_ref[...]).astype(BF16)


def matmul_nt(a, b):
    n_rows, depth = a.shape
    width = b.shape[0]
    rows, tile = n_rows // 2, tile_of(width, 1024)
    return pl.pallas_call(
        matmul_nt_kernel, grid=(2, width // tile),
        in_specs=[pl.BlockSpec((rows, depth), lambda i, j: (i, 0)), pl.BlockSpec((tile, depth), lambda i, j: (j, 0))],
        out_specs=pl.BlockSpec((rows, tile), lambda i, j: (i, j)),
        out_shape=jax.ShapeDtypeStruct((n_rows, width), BF16),
        compiler_params=COMPILER_PARAMS,
        cost_estimate=cost(2 * n_rows * depth * width),
        name="matmul_nt",
    )(a, b)


def wgrad_kernel(side_ref, *refs):
    *lhs, d0_ref, d1_ref, o_ref = refs
    part = d0_ref.shape[0] // 2
    if len(lhs) == 1:
        blocks = [lhs[0][i * part:(i + 1) * part, :] for i in range(4)]
    else:
        blocks = [lhs[0][:part, :], lhs[0][part:, :], lhs[1][...], lhs[2][...]]
    o_ref[...] = (dot_tn(blocks[0], d0_ref[:part, :]) + dot_tn(blocks[1], d1_ref[:part, :])
                  + dot_tn(blocks[2], d0_ref[part:, :]) + dot_tn(blocks[3], d1_ref[part:, :]))


def wgrad(side, lhs, d0, d1, part, n_parts):
    n_rows = d0.shape[0]
    width = d0.shape[1]
    n_cols = width // n_parts
    tall, wide = tile_of(width, 1024), tile_of(n_cols, 512)
    shift = part * n_cols // wide
    if len(lhs) == 1:
        lhs_specs = [pl.BlockSpec((2 * n_rows, tall), lambda i, j, s: (0, i))]
    else:
        lhs_specs = [pl.BlockSpec((n_rows, tall), lambda i, j, s: (s[0], i))]
        lhs_specs += [pl.BlockSpec((n_rows // 2, tall), lambda i, j, s: (0, i))] * 2
    return pl.pallas_call(
        wgrad_kernel,
        grid_spec=pltpu.PrefetchScalarGridSpec(
            num_scalar_prefetch=1, grid=(width // tall, n_cols // wide),
            in_specs=lhs_specs + [pl.BlockSpec((n_rows, wide), lambda i, j, s: (0, shift + j))] * 2,
            out_specs=pl.BlockSpec((tall, wide), lambda i, j, s: (i, j))),
        out_shape=jax.ShapeDtypeStruct((width, n_cols), F32),
        compiler_params=COMPILER_PARAMS,
        cost_estimate=cost(4 * n_rows * width * n_cols),
        name="wgrad",
    )(side, *lhs, d0, d1)


def wgrad_pass_kernel(place_ref, *refs):
    *ins, pass_ref, keep_ref = refs
    step, half = pl.program_id(1), pl.num_programs(1) // 2
    for wanted, out_ref in ((step < half, pass_ref), (step >= half, keep_ref)):
        @pl.when(wanted)
        def _():
            wgrad_kernel(place_ref, *ins, out_ref)


def wgrad_pass(place, lhs, d0, d1, part):
    n_rows, width = d0.shape
    n_cols = width // 2
    tall = width // 8
    wide = tile_of(n_cols, 1024)
    shift = part * n_cols // wide

    def rows(i, s):
        def flipped(dev, bit, wanted):
            here = lax.rem(dev // bit, 2)
            return dev + jnp.where(wanted, bit - 2 * bit * here, 0)

        q = lax.rem(i, 4)
        dev = flipped(s[1], 1, i < 4)
        dev = flipped(dev, s[2], q < 2)
        return flipped(dev, s[3], lax.rem(q, 2) == 0)

    lhs_specs = [pl.BlockSpec((n_rows, tall), lambda j, i, s: (s[0], rows(i, s)))]
    lhs_specs += [pl.BlockSpec((n_rows // 2, tall), lambda j, i, s: (0, rows(i, s)))] * 2
    return pl.pallas_call(
        wgrad_pass_kernel,
        grid_spec=pltpu.PrefetchScalarGridSpec(
            num_scalar_prefetch=1, grid=(n_cols // wide, 8),
            in_specs=lhs_specs + [pl.BlockSpec((n_rows, wide), lambda j, i, s: (0, shift + j))] * 2,
            out_specs=[pl.BlockSpec((tall, wide), lambda j, i, s: (jnp.minimum(i, 3), j)),
                       pl.BlockSpec((tall, wide), lambda j, i, s: (jnp.maximum(i - 4, 0), j))]),
        out_shape=[jax.ShapeDtypeStruct((width // 2, n_cols), F32)] * 2,
        compiler_params=COMPILER_PARAMS, cost_estimate=cost(2 * n_rows * width * width),
        name="wgrad_pass",
    )(place, *lhs, d0, d1)


def grad_x_kernel(side_ref, dq_ref, dk_ref, dv_ref, wq_ref, wk_ref, wv_ref, gy_ref, *rest):
    total = dot_nt(dq_ref[...], wq_ref[...]) + dot_nt(dk_ref[...], wk_ref[...]) + dot_nt(dv_ref[...], wv_ref[...])
    rest[-1][...] = (total + gy_ref[...].astype(F32)).astype(BF16)


def grad_x_rows(side, chunk, slot, d, weights, gy, out_rows, into=None):
    width = d[0].shape[1]
    n_rows = d[0].shape[0] // 2
    rows, tile = tile_of(n_rows, 512), tile_of(width, 512)
    steps = n_rows // rows
    row = pl.BlockSpec((rows, width), lambda i, j, s: (slot * steps + i, 0))
    weight = pl.BlockSpec((tile, width), lambda i, j, s: (j, 0))
    place = (lambda i, s: (s[0] * N_CHUNKS + chunk) * steps + i) if slot == 0 else (lambda i, s: i)
    out = pl.BlockSpec((rows, tile), lambda i, j, s: (place(i, s), j))
    specs, args = [row] * 3 + [weight] * 3 + [out], [side, *d, *weights, gy]
    if into is not None:
        specs.append(pl.BlockSpec(memory_space=pl.ANY))
        args.append(into)
    return pl.pallas_call(
        grad_x_kernel,
        grid_spec=pltpu.PrefetchScalarGridSpec(
            num_scalar_prefetch=1, grid=(steps, width // tile), in_specs=specs, out_specs=out),
        out_shape=jax.ShapeDtypeStruct((out_rows, width), BF16),
        input_output_aliases={} if into is None else {8: 0},
        compiler_params=COMPILER_PARAMS,
        cost_estimate=cost(6 * n_rows * width * width),
        name="grad_x",
    )(*args)


def post_kernel(side_ref, a_ref, x_own_ref, x_peer_ref, gy_own_ref, gy_peer_ref, gain_ref, *rest):
    y_own_ref, y_peer_ref, ga_ref, part_ref = rest[-4:]
    step, half = pl.program_id(0), pl.num_programs(0) // 2

    @pl.when(step == 0)
    def _():
        part_ref[...] = jnp.zeros_like(part_ref)

    def run(x_ref, gy_ref, y_ref):
        def rows_step(r, carry):
            rows = pl.ds(r * ROWS, ROWS)
            a = a_ref[rows, :].astype(F32)
            inv = lax.rsqrt(jnp.mean(a * a, axis=-1, keepdims=True) + RMS_EPSILON)
            hat = a * inv
            gain = gain_ref[...]
            y_ref[rows, :] = (x_ref[rows, :].astype(F32) + hat * gain).astype(BF16)
            gy = gy_ref[rows, :].astype(F32)
            prod = gy * hat
            part_ref[...] += prod[:8] + prod[8:]
            proj = jnp.mean(prod * gain, axis=-1, keepdims=True)
            ga_ref[rows, :] = (inv * (gy * gain - hat * proj)).astype(BF16)
            return carry

        lax.fori_loop(0, a_ref.shape[0] // ROWS, rows_step, 0, unroll=4)

    @pl.when(step < half)
    def _():
        run(x_peer_ref, gy_peer_ref, y_peer_ref)

    @pl.when(step >= half)
    def _():
        run(x_own_ref, gy_own_ref, y_own_ref)


def post_norm(side, chunk, a, x, x_peer, gy, gy_peer, gain, into=None):
    n_peer, width = x_peer.shape
    block = min(256, n_peer)
    half = n_peer // block
    all_half = N_CHUNKS * half

    def peer(i, s):
        return jnp.minimum(i, half - 1), 0

    def own(i, s):
        return (s[0] * N_CHUNKS + chunk) * half + jnp.maximum(i - half, 0), 0

    def a_rows(i, s):
        return jnp.where(i < half, all_half + chunk * half + i, chunk * half + i - half), 0

    def ga_rows(i, s):
        return jnp.where(i < half, half + i, i - half), 0

    def spec(index):
        return pl.BlockSpec((block, width), index)

    specs = [spec(a_rows), spec(own), spec(peer), spec(own), spec(peer), pl.BlockSpec((1, width), lambda i, s: (0, 0))]
    args = [side, a, x, x_peer, gy, gy_peer, gain]
    if into is not None:
        specs.append(pl.BlockSpec(memory_space=pl.ANY))
        args.append(into)
    return pl.pallas_call(
        post_kernel,
        grid_spec=pltpu.PrefetchScalarGridSpec(
            num_scalar_prefetch=1, grid=(2 * half,), in_specs=specs,
            out_specs=[spec(own), spec(peer), spec(ga_rows), pl.BlockSpec((8, width), lambda i, s: (0, 0))]),
        out_shape=[jax.ShapeDtypeStruct(x.shape, BF16), jax.ShapeDtypeStruct(x_peer.shape, BF16),
                   jax.ShapeDtypeStruct((2 * n_peer, width), BF16), jax.ShapeDtypeStruct((8, width), F32)],
        input_output_aliases={} if into is None else {7: 0},
        compiler_params=COMPILER_PARAMS,
        cost_estimate=cost(n_peer * width * 4096),
        name="post_norm",
    )(*args)


def solution(mesh):
    tok_spec = P('fsdp', 'sp', None)
    row_spec = P('fsdp', None)
    vec_spec = P('fsdp')
    swap = [(0, 1), (1, 0)]

    def body(x, grad_y, wq_rows, wk_rows, wv_rows, wo_rows, gq_rows, gk_rows, gpost_rows):
        n_batch, tok_len, width = x.shape
        n_own = n_batch // 2
        n_seq = n_own // N_CHUNKS
        n_part = n_seq * tok_len
        all_rows = n_batch * tok_len
        chunks = range(N_CHUNKS)
        my_side = lax.axis_index('sp')
        side = my_side.astype(jnp.int32).reshape(1)
        peer_start = (1 - my_side) * n_own

        def send(part):
            return lax.ppermute(part, 'sp', swap)

        def fetch(array):
            parts = [lax.dynamic_slice_in_dim(array, peer_start + c * n_seq, n_seq) for c in chunks]
            return [send(parts[c]).reshape(n_part, width) for c in chunks]

        x_peer = fetch(x)
        gy_peer = fetch(grad_y)
        x_flat, gy_flat = x.reshape(all_rows, width), grad_y.reshape(all_rows, width)

        w_q, w_k, w_v, w_o = (lax.all_gather(w, 'fsdp', axis=0, tiled=True) for w in (wq_rows, wk_rows, wv_rows, wo_rows))
        gains = lax.all_gather(jnp.stack([gq_rows, gk_rows, gpost_rows]), 'fsdp', axis=1, tiled=True)
        gain_q, gain_k, gain_post = gains[0:1], gains[1:2], gains[2:3]
        cos, sin = rope_tables(2 * tok_len)

        def halves(a):
            return a.reshape(2, a.shape[0] // (2 * tok_len), tok_len, width)

        def flat(a):
            return a.reshape(-1, width)

        def project(w):
            out = matmul(side, x_flat, w, all_rows, 0, 2, own=True)
            for c in chunks:
                out = matmul(side, x_peer[c], w, all_rows, 2 + c, 1, into=out)
            return halves(out)

        q0, k0, v = project(w_q), project(w_k), project(w_v)
        o, q_rot, k_rot, inv_q, inv_k, lse = attn_fwd(side, q0, k0, v, gain_q, gain_k, cos, sin)
        a_lin = matmul(side, flat(o), w_o, all_rows, 0, 4)

        y, ga, y_peer, post_parts, grads = None, [], [], [], []
        for c in chunks:
            y, y_send, ga_c, part = post_norm(side, c, a_lin, x_flat, x_peer[c], gy_flat, gy_peer[c], gain_post, into=y)
            ga.append(ga_c)
            post_parts.append(part)
            y_peer.append(send(y_send.reshape(n_seq, tok_len, width)))
        y = y.reshape(x.shape)
        for c in chunks:
            y = lax.dynamic_update_slice_in_dim(y, y_peer[c], peer_start + c * n_seq, 0)

        for c in chunks:
            d_o = halves(matmul_nt(ga[c], w_o))
            grads.append(attn_bwd(side, c, q_rot, k_rot, v, d_o, q0, k0, inv_q, inv_k, lse, gain_q, gain_k,
                                  cos * HEAD_DIM ** -0.5, sin * HEAD_DIM ** -0.5))

        def weight_grad(lhs, d, n_parts=1):
            out = []
            for i in range(n_parts):
                part = wgrad(side, lhs, *d, i, n_parts)
                rows = lax.psum_scatter(part, 'fsdp', scatter_dimension=0, tiled=True)
                out.append(rows + send(rows))
            return out[0] if n_parts == 1 else jnp.concatenate(out, axis=1)

        d_q, d_k, d_v = ([flat(g[i]) for g in grads] for i in range(3))
        g_wo = weight_grad((flat(o),), ga)
        g_wv = weight_grad((x_flat, *x_peer), d_v)
        g_wk = weight_grad((x_flat, *x_peer), d_k)

        def exchange(part, flip):
            return lax.ppermute(part, 'fsdp', [(d, d ^ flip) for d in range(8)])

        my_dev = lax.axis_index('fsdp').astype(jnp.int32)
        quarter = width // 8
        flips = ((4, 2), (2, 4))
        halves_wq = []
        for i, flip in enumerate(flips):
            place = jnp.stack([side[0], my_dev, jnp.int32(flip[0]), jnp.int32(flip[1])])
            away, keep = wgrad_pass(place, (x_flat, *x_peer), *d_q, i)
            halves_wq.append((keep, exchange(away, 1)))
        for i, (keep, near) in enumerate(halves_wq):
            half = 2 * quarter
            far = exchange(keep[:half] + near[:half], flips[i][0])
            halves_wq[i] = keep[half:], near[half:], far
        for i, parts in enumerate(halves_wq):
            last = exchange(sum(p[:quarter] for p in parts), flips[i][1])
            halves_wq[i] = sum(p[quarter:] for p in parts) + last
        g_wq = jnp.concatenate([rows + send(rows) for rows in halves_wq], axis=1)

        gx_peer, grad_x = [], None
        for c in chunks:
            gx = grad_x_rows(side, c, 1, (d_q[c], d_k[c], d_v[c]), (w_q, w_k, w_v), gy_peer[c], n_part)
            gx_peer.append(send(gx.reshape(n_seq, tok_len, width)))
        for c in chunks:
            grad_x = grad_x_rows(side, c, 0, (d_q[c], d_k[c], d_v[c]), (w_q, w_k, w_v), gy_flat, all_rows, into=grad_x)
        grad_x = grad_x.reshape(x.shape)
        for c in chunks:
            grad_x = lax.dynamic_update_slice_in_dim(grad_x, gx_peer[c], peer_start + c * n_seq, 0)

        parts = jnp.stack([sum(g[3] for g in grads).sum(0), sum(g[4] for g in grads).sum(0), sum(post_parts).sum(0)])
        for axis, flip in (("sp", 1), ("fsdp", 1), ("fsdp", 2), ("fsdp", 4)):
            parts = parts + lax.ppermute(parts, axis, [(d, d ^ flip) for d in range(mesh.shape[axis])])
        n_vec = gq_rows.shape[0]
        g_vec = lax.dynamic_slice_in_dim(parts, lax.axis_index('fsdp') * n_vec, n_vec, axis=1)
        return y, grad_x, g_wq, g_wk, g_wv, g_wo, g_vec[0], g_vec[1], g_vec[2]

    specs = (tok_spec, tok_spec, row_spec, row_spec, row_spec, row_spec, vec_spec, vec_spec, vec_spec)
    return jax.shard_map(body, mesh=mesh, in_specs=specs, out_specs=specs, check_vma=False)
```

```python
import functools

import jax
import jax.numpy as jnp
from jax import lax
from jax.experimental import pallas as pl
from jax.experimental.pallas import tpu as pltpu
from jax.sharding import PartitionSpec as P


HEAD_DIM = 128
RMS_EPSILON = 1e-6
ROPE_THETA = 500000.0
LOG2E = 1.4426950408889634
N_CHUNKS = 2
F32 = jnp.float32
BF16 = jnp.bfloat16
VMEM_BYTES = 58 * 1024 * 1024
ROWS = 16

COMPILER_PARAMS = pltpu.CompilerParams(vmem_limit_bytes=VMEM_BYTES)


def cost(flops):
    return pl.CostEstimate(flops=flops, transcendentals=0, bytes_accessed=flops // 500)


def rope_tables(seq_len):
    half_dim = HEAD_DIM // 2
    inv_freq = ROPE_THETA ** (-jnp.arange(half_dim, dtype=F32) * (2.0 / HEAD_DIM))
    angles = jnp.arange(seq_len).astype(F32)[:, None] * inv_freq[None, :]
    cos, sin = jnp.cos(angles), jnp.sin(angles)
    return jnp.concatenate([cos, cos], axis=1), jnp.concatenate([-sin, sin], axis=1)


def dot_nn(a, b):
    return lax.dot_general(a, b, (((1,), (0,)), ((), ())), preferred_element_type=F32)


def dot_nt(a, b):
    return lax.dot_general(a, b, (((1,), (1,)), ((), ())), preferred_element_type=F32)


def dot_tn(a, b):
    return lax.dot_general(a, b, (((0,), (0,)), ((), ())), preferred_element_type=F32)


def head_cols(h):
    return pl.ds(pl.multiple_of(h * HEAD_DIM, HEAD_DIM), HEAD_DIM)


def run_heads(n_heads, stages):
    depth = len(stages)

    def step(h, parity, lo, hi):
        for d in reversed(range(depth)):
            if lo <= d <= hi:
                stages[d](h - d, (parity + d) % 2)

    for h in range(depth - 1):
        step(h, h % 2, 0, h)

    def pair(i, carry):
        h = 2 * i + depth - 1
        step(h, (depth - 1) % 2, 0, depth)
        step(h + 1, depth % 2, 0, depth)
        return carry

    n_full = n_heads - (depth - 1)
    lax.fori_loop(0, n_full // 2, pair, 0)
    for h in range(depth - 1 + n_full // 2 * 2, n_heads):
        step(h, h % 2, 0, depth)
    for h in range(n_heads, n_heads + depth - 1):
        step(h, h % 2, h - n_heads + 1, depth)


def seen_pieces(half, c, part, tok_len):
    diagonal = 2 * half
    pieces = [(1, 0, tok_len)] if half else []
    if c:
        pieces.append((diagonal, 0, c))
    return pieces + [(diagonal, c, c + part)]


def store_scores(out, a_lo, a_hi, b_lo, b_hi, part):
    for block, a, b in ((0, a_lo, b_lo), (2, a_hi, b_hi)):
        for c in range(0, a.shape[0], part):
            out[block, c:c + part, c:] = dot_nt(a[c:c + part], b[c:])
    out[1] = dot_nt(a_lo, b_hi)


def clear_unseen(bufs, part):
    @pl.when(pl.program_id(0) == 0)
    def _():
        for buf in bufs:
            for block in (0, 2):
                for c in range(part, buf.shape[1], part):
                    buf[block, c:c + part, :c] = jnp.zeros((part, c), buf.dtype)


def pick_halves(side, own, peer):
    mine_first = side == 0
    return jnp.where(mine_first, own, peer), jnp.where(mine_first, peer, own)


def attn_fwd_kernel(side_ref, q0_ref, k0_ref, v_ref, gq_ref, gk_ref, cos_ref, sin_ref,
                    o_ref, qr_ref, kr_ref, iq_ref, ik_ref, lse_ref, s_bufs, p_bufs):
    side = side_ref[0]
    tok_len, width = q0_ref.shape[2], q0_ref.shape[3]
    n_heads = width // HEAD_DIM
    scale = LOG2E * HEAD_DIM ** -0.5
    first, second = side, 1 - side

    def stats(r, carry):
        rows = pl.ds(r * ROWS, ROWS)
        for src, dst in ((q0_ref, iq_ref), (k0_ref, ik_ref)):
            for slot in range(2):
                vals = src[slot, 0, rows, :].astype(F32)
                inv = lax.rsqrt(jnp.mean(vals * vals, axis=-1, keepdims=True) + RMS_EPSILON)
                dst[slot, 0, rows, :] = jnp.broadcast_to(inv, (ROWS, HEAD_DIM))
        return carry

    lax.fori_loop(0, tok_len // ROWS, stats, 0, unroll=4 if tok_len >= 4 * ROWS else 1)
    part = min(128, tok_len)
    keep = (lax.broadcasted_iota(jnp.int32, (part, part), 0) <= lax.broadcasted_iota(jnp.int32, (part, part), 1))
    clear_unseen(p_bufs, part)

    def scores(h, parity):
        cols = head_cols(h)
        rot = []
        for src, inv, gain, dst in ((q0_ref, iq_ref, gq_ref, qr_ref), (k0_ref, ik_ref, gk_ref, kr_ref)):
            slots = []
            for slot in range(2):
                pos = pl.ds(pl.multiple_of((side if slot == 0 else 1 - side) * tok_len, tok_len), tok_len)
                u = src[slot, 0, :, cols].astype(F32) * inv[slot, 0, :, :] * gain[:, cols]
                slots.append((u * cos_ref[pos, :] + pltpu.roll(u, HEAD_DIM // 2, 1) * sin_ref[pos, :]).astype(BF16))
            lo, hi = pick_halves(side, *slots)
            dst[0, :tok_len, cols] = lo
            dst[0, tok_len:, cols] = hi
            rot += [lo, hi]
        q_lo, q_hi, k_lo, k_hi = rot
        store_scores(s_bufs[parity], k_lo, k_hi, q_lo, q_hi, part)

    def softmax(h, parity):
        s, p = s_bufs[parity], p_bufs[parity]
        for c in range(0, tok_len, part):
            cols = slice(c, c + part)
            for half in range(2):
                pieces = seen_pieces(half, c, part, tok_len)
                raw = [s[b, i:j, cols] for b, i, j in pieces]
                raw[-1] = jnp.where(keep, raw[-1], -1e30)
                top = functools.reduce(jnp.maximum, [jnp.max(r, axis=0, keepdims=True) for r in raw])
                prob = [jnp.exp2((r - top) * scale) for r in raw]
                total = sum(jnp.sum(r, axis=0, keepdims=True) for r in prob)
                rec = 1.0 / total
                for r, (b, i, j) in zip(prob, pieces):
                    p[b, i:j, cols] = (r * rec).astype(BF16)
                lse = top * scale + jnp.log2(total)
                lse_ref[0, h, :, half * tok_len + c:half * tok_len + c + part] = jnp.broadcast_to(lse, (8, part))

    def mix(h, parity):
        cols = head_cols(h)
        p = p_bufs[parity]
        v_lo, v_hi = v_ref[first, 0, :, cols], v_ref[second, 0, :, cols]
        o_ref[first, 0, :, cols] = dot_tn(p[0], v_lo).astype(BF16)
        o_ref[second, 0, :, cols] = (dot_tn(p[1], v_lo) + dot_tn(p[2], v_hi)).astype(BF16)

    run_heads(n_heads, (scores, softmax, mix))


def attn_fwd(side, q0, k0, v, gain_q, gain_k, cos, sin):
    _, n_seq, tok_len, width = q0.shape
    seq_len = 2 * tok_len
    halves = pl.BlockSpec((2, 1, tok_len, width), lambda j, s: (0, j, 0, 0))
    whole = pl.BlockSpec((1, seq_len, width), lambda j, s: (j, 0, 0))
    inv = pl.BlockSpec((2, 1, tok_len, HEAD_DIM), lambda j, s: (0, j, 0, 0))
    vec = pl.BlockSpec((1, width), lambda j, s: (0, 0))
    tab = pl.BlockSpec((seq_len, HEAD_DIM), lambda j, s: (0, 0))
    n_heads = width // HEAD_DIM
    square = (3, tok_len, tok_len)
    return pl.pallas_call(
        attn_fwd_kernel,
        grid_spec=pltpu.PrefetchScalarGridSpec(
            num_scalar_prefetch=1, grid=(n_seq,),
            in_specs=[halves, halves, halves, vec, vec, tab, tab],
            out_specs=[halves, whole, whole, inv, inv, pl.BlockSpec((1, n_heads, 8, seq_len), lambda j, s: (j, 0, 0, 0))],
            scratch_shapes=[[pltpu.VMEM(square, F32)] * 2, [pltpu.VMEM(square, BF16)] * 2]),
        out_shape=[jax.ShapeDtypeStruct(q0.shape, BF16)]
        + [jax.ShapeDtypeStruct((n_seq, seq_len, width), BF16)] * 2
        + [jax.ShapeDtypeStruct((2, n_seq, tok_len, HEAD_DIM), F32)] * 2 + [jax.ShapeDtypeStruct((n_seq, n_heads, 8, seq_len), F32)],
        compiler_params=COMPILER_PARAMS,
        cost_estimate=cost(12 * n_seq * seq_len * seq_len * width),
        name="attn_fwd",
    )(side, q0, k0, v, gain_q, gain_k, cos, sin)


def attn_bwd_kernel(side_ref, qr_ref, kr_ref, v_ref, do_ref, q0_ref, k0_ref, iq_ref, ik_ref, lse_ref, gq_ref, gk_ref, cos_ref, sin_ref,
                    dq_ref, dk_ref, dv_ref, gqp_ref, gkp_ref,
                    acc_q, acc_k, proj_q, proj_k, s_bufs, d_bufs, p_bufs, ds_bufs):
    side = side_ref[0]
    tok_len, width = q0_ref.shape[2], q0_ref.shape[3]
    n_heads = width // HEAD_DIM
    scale = LOG2E * HEAD_DIM ** -0.5
    first, second = side, 1 - side
    lo, hi = slice(0, tok_len), slice(tok_len, 2 * tok_len)

    @pl.when(pl.program_id(0) == 0)
    def _():
        gqp_ref[...] = jnp.zeros_like(gqp_ref)
        gkp_ref[...] = jnp.zeros_like(gkp_ref)

    part = min(128, tok_len)
    keep = (lax.broadcasted_iota(jnp.int32, (part, part), 0) <= lax.broadcasted_iota(jnp.int32, (part, part), 1))
    clear_unseen((*p_bufs, *ds_bufs), part)
    proj_q[...] = jnp.zeros_like(proj_q)
    proj_k[...] = jnp.zeros_like(proj_k)

    def scores(h, parity):
        cols = head_cols(h)
        k_lo, k_hi = kr_ref[0, lo, cols], kr_ref[0, hi, cols]
        q_lo, q_hi = qr_ref[0, lo, cols], qr_ref[0, hi, cols]
        v_lo, v_hi = v_ref[first, 0, :, cols], v_ref[second, 0, :, cols]
        do_lo, do_hi = do_ref[first, 0, :, cols], do_ref[second, 0, :, cols]
        store_scores(s_bufs[parity], k_lo, k_hi, q_lo, q_hi, part)
        store_scores(d_bufs[parity], v_lo, v_hi, do_lo, do_hi, part)

    def softmax(h, parity):
        s, d, p, ds = s_bufs[parity], d_bufs[parity], p_bufs[parity], ds_bufs[parity]
        for c in range(0, tok_len, part):
            cols = slice(c, c + part)
            for half in range(2):
                pieces = seen_pieces(half, c, part, tok_len)
                lse = lse_ref[0, h, 0:1, half * tok_len + c:half * tok_len + c + part]
                prob = [jnp.exp2(s[b, i:j, cols] * scale - lse) for b, i, j in pieces]
                prob[-1] = jnp.where(keep, prob[-1], 0.0)
                delta = sum(jnp.sum(r * d[b, i:j, cols], axis=0, keepdims=True) for r, (b, i, j) in zip(prob, pieces))
                for r, (b, i, j) in zip(prob, pieces):
                    p[b, i:j, cols] = r.astype(BF16)
                    ds[b, i:j, cols] = (r * (d[b, i:j, cols] - delta)).astype(BF16)

    def grads(h, parity):
        cols = head_cols(h)
        k_lo, k_hi = kr_ref[0, lo, cols], kr_ref[0, hi, cols]
        q_lo, q_hi = qr_ref[0, lo, cols], qr_ref[0, hi, cols]
        do_lo, do_hi = do_ref[first, 0, :, cols], do_ref[second, 0, :, cols]
        p, ds = p_bufs[parity], ds_bufs[parity]
        dv_ref[first, 0, :, cols] = (dot_nn(p[0], do_lo) + dot_nn(p[1], do_hi)).astype(BF16)
        dv_ref[second, 0, :, cols] = dot_nn(p[2], do_hi).astype(BF16)
        dq_lo = dot_tn(ds[0], k_lo)
        dq_hi = dot_tn(ds[1], k_lo) + dot_tn(ds[2], k_hi)
        dk_lo = dot_nn(ds[0], q_lo) + dot_nn(ds[1], q_hi)
        dk_hi = dot_nn(ds[2], q_hi)
        for pair, src, inv, gain, acc, proj, part_ref in (((dq_lo, dq_hi), q0_ref, iq_ref, gq_ref, acc_q, proj_q, gqp_ref),
                                                          ((dk_lo, dk_hi), k0_ref, ik_ref, gk_ref, acc_k, proj_k, gkp_ref)):
            total = jnp.zeros((8, HEAD_DIM), F32)
            for g, rows, slot in zip(pair, (lo, hi), (first, second)):
                g = (g * cos_ref[rows, :] - pltpu.roll(g, HEAD_DIM // 2, 1) * sin_ref[rows, :]) * inv[slot, 0, :, :]
                vals = src[slot, 0, :, cols].astype(F32)
                total += jnp.sum((g * vals).reshape(tok_len // 8, 8, HEAD_DIM), axis=0)
                g = g * gain[:, cols]
                proj[rows, :] += g * vals
                acc[rows, cols] = g
            part_ref[:, cols] += total

    run_heads(n_heads, (scores, softmax, grads))

    for proj, inv in ((proj_q, iq_ref), (proj_k, ik_ref)):
        for rows, slot in ((lo, first), (hi, second)):
            i = inv[slot, 0, :, :]
            proj[rows, :] = jnp.sum(proj[rows, :], axis=-1, keepdims=True) * (1.0 / width) * i * i

    def finish(r, carry):
        rows = pl.ds(r * ROWS, ROWS)
        for acc, src, proj, dst in ((acc_q, q0_ref, proj_q, dq_ref), (acc_k, k0_ref, proj_k, dk_ref)):
            for slot in range(2):
                pos = pl.ds(pl.multiple_of((side if slot == 0 else 1 - side) * tok_len + r * ROWS, ROWS), ROWS)
                c = proj[pos, :]
                for h in range(n_heads):
                    cols = slice(h * HEAD_DIM, (h + 1) * HEAD_DIM)
                    dst[slot, 0, rows, cols] = (acc[pos, cols] - src[slot, 0, rows, cols].astype(F32) * c).astype(BF16)
        return carry

    lax.fori_loop(0, tok_len // ROWS, finish, 0)


def attn_bwd(side, chunk, q_rot, k_rot, v, d_out, q0, k0, inv_q, inv_k, lse, gain_q, gain_k, cos, sin):
    _, n_seq, tok_len, width = d_out.shape
    seq_len = 2 * tok_len
    first = chunk * n_seq
    halves = pl.BlockSpec((2, 1, tok_len, width), lambda j, s: (0, first + j, 0, 0))
    part_halves = pl.BlockSpec((2, 1, tok_len, width), lambda j, s: (0, j, 0, 0))
    whole = pl.BlockSpec((1, seq_len, width), lambda j, s: (first + j, 0, 0))
    inv = pl.BlockSpec((2, 1, tok_len, HEAD_DIM), lambda j, s: (0, first + j, 0, 0))
    vec = pl.BlockSpec((1, width), lambda j, s: (0, 0))
    part = pl.BlockSpec((8, width), lambda j, s: (0, 0))
    tab = pl.BlockSpec((seq_len, HEAD_DIM), lambda j, s: (0, 0))
    n_heads = width // HEAD_DIM
    square = (3, tok_len, tok_len)
    return pl.pallas_call(
        attn_bwd_kernel,
        grid_spec=pltpu.PrefetchScalarGridSpec(
            num_scalar_prefetch=1, grid=(n_seq,),
            in_specs=[whole, whole, halves, part_halves, halves, halves, inv, inv,
                      pl.BlockSpec((1, n_heads, 8, seq_len), lambda j, s: (first + j, 0, 0, 0)), vec, vec, tab, tab],
            out_specs=[part_halves, part_halves, part_halves, part, part],
            scratch_shapes=[pltpu.VMEM((seq_len, width), F32)] * 2 + [pltpu.VMEM((seq_len, HEAD_DIM), F32)] * 2
            + [[pltpu.VMEM(square, F32)] * 2] * 2 + [[pltpu.VMEM(square, BF16)] * 2] * 2),
        out_shape=[jax.ShapeDtypeStruct(d_out.shape, BF16)] * 3 + [jax.ShapeDtypeStruct((8, width), F32)] * 2,
        compiler_params=COMPILER_PARAMS,
        cost_estimate=cost(30 * n_seq * seq_len * seq_len * width),
        name="attn_bwd",
    )(side, q_rot, k_rot, v, d_out, q0, k0, inv_q, inv_k, lse, gain_q, gain_k, cos, sin)


def tile_of(n, most):
    return most if n % most == 0 else n


def matmul_kernel(n, side_ref, a_ref, *refs):
    for m in range(n):
        @pl.when(pl.program_id(1) == m)
        def _():
            refs[m - n][...] = dot_nn(a_ref[...], refs[m][...]).astype(BF16)


def matmul(side, a, weights, out_rows, out_block, n_blocks, own=False, into=()):
    n = len(weights)
    depth, width = weights[0].shape
    rows = out_rows // 4
    tile = tile_of(width, 1024 if n == 1 else 512)

    def row_block(i, k, j, s):
        return s[0] * n_blocks + i if own else i, 0

    def columns(m, k, j):
        return jnp.where(k == m, j, jnp.where(k < m, 0, width // tile - 1))

    specs = [pl.BlockSpec((rows, depth), row_block)]
    specs += [pl.BlockSpec((depth, tile), lambda i, k, j, s, m=m: (0, columns(m, k, j))) for m in range(n)]
    specs += [pl.BlockSpec(memory_space=pl.ANY)] * len(into)
    return pl.pallas_call(
        functools.partial(matmul_kernel, n),
        grid_spec=pltpu.PrefetchScalarGridSpec(
            num_scalar_prefetch=1, grid=(n_blocks, n, width // tile), in_specs=specs,
            out_specs=[pl.BlockSpec((rows, tile), lambda i, k, j, s, m=m: (out_block + i, columns(m, k, j))) for m in range(n)]),
        out_shape=[jax.ShapeDtypeStruct((out_rows, width), BF16)] * n,
        input_output_aliases={2 + n + m: m for m in range(len(into))},
        compiler_params=COMPILER_PARAMS, cost_estimate=cost(2 * n * n_blocks * rows * depth * width),
        name="matmul",
    )(side, a, *weights, *into)


def matmul_nt_kernel(a_ref, b_ref, o_ref):
    o_ref[...] = dot_nt(a_ref[...], b_ref[...]).astype(BF16)


def matmul_nt(a, b):
    n_rows, depth = a.shape
    width = b.shape[0]
    rows, tile = n_rows // 2, tile_of(width, 1024)
    return pl.pallas_call(
        matmul_nt_kernel, grid=(2, width // tile),
        in_specs=[pl.BlockSpec((rows, depth), lambda i, j: (i, 0)), pl.BlockSpec((tile, depth), lambda i, j: (j, 0))],
        out_specs=pl.BlockSpec((rows, tile), lambda i, j: (i, j)),
        out_shape=jax.ShapeDtypeStruct((n_rows, width), BF16),
        compiler_params=COMPILER_PARAMS,
        cost_estimate=cost(2 * n_rows * depth * width),
        name="matmul_nt",
    )(a, b)


def wgrad_kernel(side_ref, *refs):
    *lhs, d0_ref, d1_ref, o_ref = refs
    part = d0_ref.shape[0] // 2
    if len(lhs) == 1:
        blocks = [lhs[0][i * part:(i + 1) * part, :] for i in range(4)]
    else:
        blocks = [lhs[0][:part, :], lhs[0][part:, :], lhs[1][...], lhs[2][...]]
    o_ref[...] = (dot_tn(blocks[0], d0_ref[:part, :]) + dot_tn(blocks[1], d1_ref[:part, :])
                  + dot_tn(blocks[2], d0_ref[part:, :]) + dot_tn(blocks[3], d1_ref[part:, :]))


def wgrad(side, lhs, d0, d1, part, n_parts):
    n_rows = d0.shape[0]
    width = d0.shape[1]
    n_cols = width // n_parts
    tall, wide = tile_of(width, 1024), tile_of(n_cols, 512)
    shift = part * n_cols // wide
    if len(lhs) == 1:
        lhs_specs = [pl.BlockSpec((2 * n_rows, tall), lambda i, j, s: (0, i))]
    else:
        lhs_specs = [pl.BlockSpec((n_rows, tall), lambda i, j, s: (s[0], i))]
        lhs_specs += [pl.BlockSpec((n_rows // 2, tall), lambda i, j, s: (0, i))] * 2
    return pl.pallas_call(
        wgrad_kernel,
        grid_spec=pltpu.PrefetchScalarGridSpec(
            num_scalar_prefetch=1, grid=(width // tall, n_cols // wide),
            in_specs=lhs_specs + [pl.BlockSpec((n_rows, wide), lambda i, j, s: (0, shift + j))] * 2,
            out_specs=pl.BlockSpec((tall, wide), lambda i, j, s: (i, j))),
        out_shape=jax.ShapeDtypeStruct((width, n_cols), F32),
        compiler_params=COMPILER_PARAMS,
        cost_estimate=cost(4 * n_rows * width * n_cols),
        name="wgrad",
    )(side, *lhs, d0, d1)


def wgrad_pass_kernel(place_ref, *refs):
    *ins, pass_ref, keep_ref = refs
    step, half = pl.program_id(1), pl.num_programs(1) // 2
    for wanted, out_ref in ((step < half, pass_ref), (step >= half, keep_ref)):
        @pl.when(wanted)
        def _():
            wgrad_kernel(place_ref, *ins, out_ref)


def wgrad_pass(place, lhs, d0, d1, part):
    n_rows, width = d0.shape
    n_cols = width // 2
    tall = width // 8
    wide = tile_of(n_cols, 1024)
    shift = part * n_cols // wide

    def rows(i, s):
        def flipped(dev, bit, wanted):
            here = lax.rem(dev // bit, 2)
            return dev + jnp.where(wanted, bit - 2 * bit * here, 0)

        q = lax.rem(i, 4)
        dev = flipped(s[1], 1, i < 4)
        dev = flipped(dev, s[2], q < 2)
        return flipped(dev, s[3], lax.rem(q, 2) == 0)

    lhs_specs = [pl.BlockSpec((n_rows, tall), lambda j, i, s: (s[0], rows(i, s)))]
    lhs_specs += [pl.BlockSpec((n_rows // 2, tall), lambda j, i, s: (0, rows(i, s)))] * 2
    return pl.pallas_call(
        wgrad_pass_kernel,
        grid_spec=pltpu.PrefetchScalarGridSpec(
            num_scalar_prefetch=1, grid=(n_cols // wide, 8),
            in_specs=lhs_specs + [pl.BlockSpec((n_rows, wide), lambda j, i, s: (0, shift + j))] * 2,
            out_specs=[pl.BlockSpec((tall, wide), lambda j, i, s: (jnp.minimum(i, 3), j)),
                       pl.BlockSpec((tall, wide), lambda j, i, s: (jnp.maximum(i - 4, 0), j))]),
        out_shape=[jax.ShapeDtypeStruct((width // 2, n_cols), F32)] * 2,
        compiler_params=COMPILER_PARAMS, cost_estimate=cost(2 * n_rows * width * width),
        name="wgrad_pass",
    )(place, *lhs, d0, d1)


def grad_x_kernel(side_ref, dq_ref, dk_ref, dv_ref, wq_ref, wk_ref, wv_ref, gy_ref, *rest):
    total = dot_nt(dq_ref[...], wq_ref[...]) + dot_nt(dk_ref[...], wk_ref[...]) + dot_nt(dv_ref[...], wv_ref[...])
    rest[-1][...] = (total + gy_ref[...].astype(F32)).astype(BF16)


def grad_x_rows(side, chunk, slot, d, weights, gy, out_rows, into=None):
    width = d[0].shape[1]
    n_rows = d[0].shape[0] // 2
    rows, tile = tile_of(n_rows, 512), tile_of(width, 512)
    steps = n_rows // rows
    row = pl.BlockSpec((rows, width), lambda i, j, s: (slot * steps + i, 0))
    weight = pl.BlockSpec((tile, width), lambda i, j, s: (j, 0))
    place = (lambda i, s: (s[0] * N_CHUNKS + chunk) * steps + i) if slot == 0 else (lambda i, s: i)
    out = pl.BlockSpec((rows, tile), lambda i, j, s: (place(i, s), j))
    specs, args = [row] * 3 + [weight] * 3 + [out], [side, *d, *weights, gy]
    if into is not None:
        specs.append(pl.BlockSpec(memory_space=pl.ANY))
        args.append(into)
    return pl.pallas_call(
        grad_x_kernel,
        grid_spec=pltpu.PrefetchScalarGridSpec(
            num_scalar_prefetch=1, grid=(steps, width // tile), in_specs=specs, out_specs=out),
        out_shape=jax.ShapeDtypeStruct((out_rows, width), BF16),
        input_output_aliases={} if into is None else {8: 0},
        compiler_params=COMPILER_PARAMS,
        cost_estimate=cost(6 * n_rows * width * width),
        name="grad_x",
    )(*args)


def post_kernel(side_ref, a_ref, x_own_ref, x_peer_ref, gy_own_ref, gy_peer_ref, gain_ref, *rest):
    y_own_ref, y_peer_ref, ga_ref, part_ref = rest[-4:]
    step, half = pl.program_id(0), pl.num_programs(0) // 2

    @pl.when(step == 0)
    def _():
        part_ref[...] = jnp.zeros_like(part_ref)

    def run(x_ref, gy_ref, y_ref):
        def rows_step(r, carry):
            rows = pl.ds(r * ROWS, ROWS)
            a = a_ref[rows, :].astype(F32)
            inv = lax.rsqrt(jnp.mean(a * a, axis=-1, keepdims=True) + RMS_EPSILON)
            hat = a * inv
            gain = gain_ref[...]
            y_ref[rows, :] = (x_ref[rows, :].astype(F32) + hat * gain).astype(BF16)
            gy = gy_ref[rows, :].astype(F32)
            prod = gy * hat
            part_ref[...] += prod[:8] + prod[8:]
            proj = jnp.mean(prod * gain, axis=-1, keepdims=True)
            ga_ref[rows, :] = (inv * (gy * gain - hat * proj)).astype(BF16)
            return carry

        lax.fori_loop(0, a_ref.shape[0] // ROWS, rows_step, 0, unroll=4)

    @pl.when(step < half)
    def _():
        run(x_peer_ref, gy_peer_ref, y_peer_ref)

    @pl.when(step >= half)
    def _():
        run(x_own_ref, gy_own_ref, y_own_ref)


def post_norm(side, chunk, a, x, x_peer, gy, gy_peer, gain, into=None):
    n_peer, width = x_peer.shape
    block = min(256, n_peer)
    half = n_peer // block
    all_half = N_CHUNKS * half

    def peer(i, s):
        return jnp.minimum(i, half - 1), 0

    def own(i, s):
        return (s[0] * N_CHUNKS + chunk) * half + jnp.maximum(i - half, 0), 0

    def a_rows(i, s):
        return jnp.where(i < half, all_half + chunk * half + i, chunk * half + i - half), 0

    def ga_rows(i, s):
        return jnp.where(i < half, half + i, i - half), 0

    def spec(index):
        return pl.BlockSpec((block, width), index)

    specs = [spec(a_rows), spec(own), spec(peer), spec(own), spec(peer), pl.BlockSpec((1, width), lambda i, s: (0, 0))]
    args = [side, a, x, x_peer, gy, gy_peer, gain]
    if into is not None:
        specs.append(pl.BlockSpec(memory_space=pl.ANY))
        args.append(into)
    return pl.pallas_call(
        post_kernel,
        grid_spec=pltpu.PrefetchScalarGridSpec(
            num_scalar_prefetch=1, grid=(2 * half,), in_specs=specs,
            out_specs=[spec(own), spec(peer), spec(ga_rows), pl.BlockSpec((8, width), lambda i, s: (0, 0))]),
        out_shape=[jax.ShapeDtypeStruct(x.shape, BF16), jax.ShapeDtypeStruct(x_peer.shape, BF16),
                   jax.ShapeDtypeStruct((2 * n_peer, width), BF16), jax.ShapeDtypeStruct((8, width), F32)],
        input_output_aliases={} if into is None else {7: 0},
        compiler_params=COMPILER_PARAMS,
        cost_estimate=cost(n_peer * width * 4096),
        name="post_norm",
    )(*args)


def solution(mesh):
    tok_spec = P('fsdp', 'sp', None)
    row_spec = P('fsdp', None)
    vec_spec = P('fsdp')
    swap = [(0, 1), (1, 0)]

    def body(x, grad_y, wq_rows, wk_rows, wv_rows, wo_rows, gq_rows, gk_rows, gpost_rows):
        n_batch, tok_len, width = x.shape
        n_own = n_batch // 2
        n_seq = n_own // N_CHUNKS
        n_part = n_seq * tok_len
        all_rows = n_batch * tok_len
        chunks = range(N_CHUNKS)
        my_side = lax.axis_index('sp')
        side = my_side.astype(jnp.int32).reshape(1)
        peer_start = (1 - my_side) * n_own

        def send(part):
            return lax.ppermute(part, 'sp', swap)

        def fetch(array):
            parts = [lax.dynamic_slice_in_dim(array, peer_start + c * n_seq, n_seq) for c in chunks]
            return [send(parts[c]).reshape(n_part, width) for c in chunks]

        x_peer = fetch(x)
        gy_peer = fetch(grad_y)
        x_flat, gy_flat = x.reshape(all_rows, width), grad_y.reshape(all_rows, width)

        w_q, w_k, w_v, w_o = (lax.all_gather(w, 'fsdp', axis=0, tiled=True) for w in (wq_rows, wk_rows, wv_rows, wo_rows))
        gains = lax.all_gather(jnp.stack([gq_rows, gk_rows, gpost_rows]), 'fsdp', axis=1, tiled=True)
        gain_q, gain_k, gain_post = gains[0:1], gains[1:2], gains[2:3]
        cos, sin = rope_tables(2 * tok_len)

        def halves(a):
            return a.reshape(2, a.shape[0] // (2 * tok_len), tok_len, width)

        def flat(a):
            return a.reshape(-1, width)

        def project(a, weights, out_block, into=()):
            return matmul(side, a, weights, all_rows, out_block, 1 if into else 2, own=not into, into=into)

        q0, = project(x_flat, (w_q,), 0)
        k0, = project(x_flat, (w_k,), 0)
        v, = project(x_flat, (w_v,), 0)
        q0, k0 = project(x_peer[0], (w_q, w_k), 2, (q0, k0))
        v, = project(x_peer[0], (w_v,), 2, (v,))
        q0, k0, v = map(halves, project(x_peer[1], (w_q, w_k, w_v), 3, (q0, k0, v)))
        o, q_rot, k_rot, inv_q, inv_k, lse = attn_fwd(side, q0, k0, v, gain_q, gain_k, cos, sin)
        a_lin, = matmul(side, flat(o), (w_o,), all_rows, 0, 4)

        y, ga, y_peer, post_parts, grads = None, [], [], [], []
        for c in chunks:
            y, y_send, ga_c, part = post_norm(side, c, a_lin, x_flat, x_peer[c], gy_flat, gy_peer[c], gain_post, into=y)
            ga.append(ga_c)
            post_parts.append(part)
            y_peer.append(send(y_send.reshape(n_seq, tok_len, width)))
        y = y.reshape(x.shape)
        for c in chunks:
            y = lax.dynamic_update_slice_in_dim(y, y_peer[c], peer_start + c * n_seq, 0)

        for c in chunks:
            d_o = halves(matmul_nt(ga[c], w_o))
            grads.append(attn_bwd(side, c, q_rot, k_rot, v, d_o, q0, k0, inv_q, inv_k, lse, gain_q, gain_k,
                                  cos * HEAD_DIM ** -0.5, sin * HEAD_DIM ** -0.5))

        def weight_grad(lhs, d, n_parts=1):
            out = []
            for i in range(n_parts):
                part = wgrad(side, lhs, *d, i, n_parts)
                rows = lax.psum_scatter(part, 'fsdp', scatter_dimension=0, tiled=True)
                out.append(rows + send(rows))
            return out[0] if n_parts == 1 else jnp.concatenate(out, axis=1)

        d_q, d_k, d_v = ([flat(g[i]) for g in grads] for i in range(3))
        g_wo = weight_grad((flat(o),), ga)
        g_wv = weight_grad((x_flat, *x_peer), d_v)
        g_wk = weight_grad((x_flat, *x_peer), d_k, 2)

        def exchange(part, flip):
            return lax.ppermute(part, 'fsdp', [(d, d ^ flip) for d in range(8)])

        my_dev = lax.axis_index('fsdp').astype(jnp.int32)
        quarter = width // 8
        flips = ((4, 2), (2, 4))
        halves_wq = []
        for i, flip in enumerate(flips):
            place = jnp.stack([side[0], my_dev, jnp.int32(flip[0]), jnp.int32(flip[1])])
            away, keep = wgrad_pass(place, (x_flat, *x_peer), *d_q, i)
            halves_wq.append((keep, exchange(away, 1)))
        for i, (keep, near) in enumerate(halves_wq):
            half = 2 * quarter
            far = exchange(keep[:half] + near[:half], flips[i][0])
            halves_wq[i] = keep[half:], near[half:], far
        for i, parts in enumerate(halves_wq):
            last = exchange(sum(p[:quarter] for p in parts), flips[i][1])
            halves_wq[i] = sum(p[quarter:] for p in parts) + last
        g_wq = jnp.concatenate([rows + send(rows) for rows in halves_wq], axis=1)

        gx_peer, grad_x = [], None
        for c in chunks:
            gx = grad_x_rows(side, c, 1, (d_q[c], d_k[c], d_v[c]), (w_q, w_k, w_v), gy_peer[c], n_part)
            gx_peer.append(send(gx.reshape(n_seq, tok_len, width)))
        for c in chunks:
            grad_x = grad_x_rows(side, c, 0, (d_q[c], d_k[c], d_v[c]), (w_q, w_k, w_v), gy_flat, all_rows, into=grad_x)
        grad_x = grad_x.reshape(x.shape)
        for c in chunks:
            grad_x = lax.dynamic_update_slice_in_dim(grad_x, gx_peer[c], peer_start + c * n_seq, 0)

        parts = jnp.stack([sum(g[3] for g in grads).sum(0), sum(g[4] for g in grads).sum(0), sum(post_parts).sum(0)])
        for axis, flip in (("sp", 1), ("fsdp", 1), ("fsdp", 2), ("fsdp", 4)):
            parts = parts + lax.ppermute(parts, axis, [(d, d ^ flip) for d in range(mesh.shape[axis])])
        n_vec = gq_rows.shape[0]
        g_vec = lax.dynamic_slice_in_dim(parts, lax.axis_index('fsdp') * n_vec, n_vec, axis=1)
        return y, grad_x, g_wq, g_wk, g_wv, g_wo, g_vec[0], g_vec[1], g_vec[2]

    specs = (tok_spec, tok_spec, row_spec, row_spec, row_spec, row_spec, vec_spec, vec_spec, vec_spec)
    return jax.shard_map(body, mesh=mesh, in_specs=specs, out_specs=specs, check_vma=False)
```
